128 devices in a mesh: south: 4 (over x), east: 8 (over y, core), down: 4 (over z).
Axes of the slice: x: 4, y: 4, z: 4, core: 2. Of those that a mesh axis runs over, the one named last changes fastest.
Arguments:
- field_now: float32 [32, 128, 512, 128], P('south', 'east', 'down'), may hold values from 0.2 to 1.8
- earlier: float32 [32, 128, 512, 128], P('south', 'east', 'down'), may hold values from 0.2 to 1.8
- speed_square: float32 [32, 128, 512, 128], P('south', 'east', 'down'), may hold values from 0.05 to 0.3
Outputs:
- running_total: float32 [32, 128, 512, 128], P('south', 'east', 'down')
- field_now_end: float32 [32, 128, 512, 128], P('south', 'east', 'down')
The draws below stay inside these ranges and needn't reach their ends.
All inputs are finite; a program needn't handle non-finite values.
Results may differ from the reference program's by a relative error of at most 0.00002.
Values sent between devices are 32-bit elements; how exact they have to be, the bound alone decides.
A program may use at most 320 MiB of HBM per device.

```python
import jax
import jax.numpy as jnp
from jax import lax

GRID_J = 32
GRID_I = 128
GRID_K = 512
MEMBERS = 128
STEPS = 4


def levels(stream_key, shape, cuts, smallest, largest):
    loudness = 1.0
    for dim, blocks in cuts:
        draws = jax.random.uniform(jax.random.fold_in(jax.random.fold_in(stream_key, 6), dim), (blocks,), jnp.float32, smallest / len(cuts), largest / len(cuts))
        loudness = loudness * jnp.repeat(jnp.exp(draws), shape[dim] // blocks).reshape((-1,) + (1,) * (len(shape) - 1 - dim))
    return loudness


def setup_inputs(seed: int = 0) -> dict:
    key_list = jax.random.split(jax.random.key(seed), 4)
    field_now = jnp.clip(0.2 + 1.5999999 * jax.random.uniform(key_list[0], (GRID_J, GRID_I, GRID_K, MEMBERS), jnp.float32) ** levels(key_list[0], (GRID_J, GRID_I, GRID_K, MEMBERS), ((0, 4), (1, 8), (2, 4)), -0.2, 0.2), 0.2, 1.8)
    earlier = jnp.clip(0.2 + 1.5999999 * jax.random.uniform(key_list[1], (GRID_J, GRID_I, GRID_K, MEMBERS), jnp.float32) ** levels(key_list[1], (GRID_J, GRID_I, GRID_K, MEMBERS), ((0, 4), (1, 8), (2, 4)), -0.2, 0.2), 0.2, 1.8)
    speed_square = jnp.clip(0.05 + 0.25 * jax.random.uniform(key_list[2], (GRID_J, GRID_I, GRID_K, MEMBERS), jnp.float32) ** levels(key_list[2], (GRID_J, GRID_I, GRID_K, MEMBERS), ((0, 4), (1, 8), (2, 4)), -0.2, 0.2), 0.05, 0.3)
    return {"field_now": field_now, "earlier": earlier, "speed_square": speed_square}


def strip_edges(values, dims):
    for dim in dims:
        values = lax.slice_in_dim(values, 1, values.shape[dim] - 1, axis=dim)
    return values


def neighbour(values, dim, start, dims):
    others = [other for other in dims if other != dim]
    values = strip_edges(values, others)
    return lax.slice_in_dim(values, start, start + values.shape[dim] - 2, axis=dim)


def one_step(padded, before, speed_square):
    middle = strip_edges(padded, (0, 1, 2))
    lower = [neighbour(padded, dim, 0, (0, 1, 2)) for dim in (0, 1, 2)]
    upper = [neighbour(padded, dim, 2, (0, 1, 2)) for dim in (0, 1, 2)]
    spread = lower[0] + upper[0] + lower[1] + upper[1] + lower[2] + upper[2] - 6.0 * middle
    return 2.0 * middle - before + speed_square * spread


def reference(field_now, earlier, speed_square):
    for step in range(STEPS):
        later = one_step(jnp.pad(field_now, ((1, 1), (1, 1), (1, 1), (0, 0)), mode="constant"), earlier, speed_square)
        earlier, field_now = field_now, later
    running_total = jnp.cumsum(field_now, axis=0) / GRID_J
    return running_total, field_now
```

```python
import functools

import jax
import jax.numpy as jnp
from jax import lax
from jax.experimental import pallas as pl
from jax.experimental.pallas import tpu as pltpu
from jax.sharding import PartitionSpec as P

STEPS = 4
ROWS = 4
AXES = ("south", "east", "down")


def steps_kernel(
    grid_j, u0, e0, s0, field, below, prev, speed, zsend, zrecv, total,
    load_sem, xsend_sem, xrecv_sem, ysend_sem, yrecv_sem, zsend_sem, zrecv_sem, tsend_sem, trecv_sem,
):
    nj, ni, nk, nm = s0.shape
    chunks = ni // ROWS
    place = {a: lax.axis_index(a) for a in AXES}
    count = {a: lax.axis_size(a) for a in AXES}
    has = {a: (place[a] > 0, place[a] < count[a] - 1) for a in AXES}
    peer = {a: (place[a] - 1, place[a] + 1) for a in AXES}

    inner = (pl.ds(1, nj), pl.ds(1, ni))
    loads = [
        pltpu.make_async_copy(u0, field.at[inner], load_sem.at[0]),
        pltpu.make_async_copy(e0, prev.at[inner], load_sem.at[1]),
        pltpu.make_async_copy(s0, speed, load_sem.at[2]),
    ]
    for load in loads:
        load.start()

    barrier = pltpu.get_barrier_semaphore()
    greeted = 0
    for a in AXES:
        for side in (0, 1):
            @pl.when(has[a][side])
            def _():
                pl.semaphore_signal(barrier, inc=1, device_id={a: peer[a][side]}, device_id_type=pl.DeviceIdType.MESH)
            greeted = greeted + has[a][side].astype(jnp.int32)
    pl.semaphore_wait(barrier, greeted)

    bufs = (field, prev)

    def remote(src, dst, send_sem, recv_sem, axis, side):
        return pltpu.make_async_remote_copy(
            src_ref=src, dst_ref=dst, send_sem=send_sem, recv_sem=recv_sem,
            device_id={axis: peer[axis][side]}, device_id_type=pl.DeviceIdType.MESH,
        )

    def x_copy(t, side, c, src=None):
        buf = bufs[t % 2]
        rows = pl.ds(1 + c * ROWS, ROWS)
        own, dst = (nj if side else 1), (0 if side else nj + 1)
        src = buf.at[own, rows] if src is None else src
        return remote(src, buf.at[dst, rows], xsend_sem.at[t, side, c], xrecv_sem.at[t, 1 - side, c], "south", side)

    def y_copy(t, side, src=None):
        buf = bufs[t % 2]
        own, dst = (ni if side else 1), (0 if side else ni + 1)
        src = buf.at[pl.ds(1, nj), own] if src is None else src
        return remote(src, buf.at[pl.ds(1, nj), dst], ysend_sem.at[t, side], yrecv_sem.at[t, 1 - side], "east", side)

    def z_copy(t, side, c):
        rows = pl.ds(c * ROWS, ROWS)
        return remote(
            zsend.at[t, side, rows], zrecv.at[t, 1 - side, rows],
            zsend_sem.at[t, side, c], zrecv_sem.at[t, 1 - side, c], "down", side,
        )

    def on(pred, action):
        @pl.when(pred)
        def _():
            action()

    for c in range(chunks):
        rows = pl.ds(c * ROWS, ROWS)
        for side in (1, 0):
            on(has["south"][side], lambda: x_copy(0, side, c, u0.at[nj - 1 if side else 0, rows]).start())
    for side in (1, 0):
        on(has["east"][side], lambda: y_copy(0, side, u0.at[:, ni - 1 if side else 0]).start())

    for buf in bufs:
        for side in (0, 1):
            @pl.when(jnp.logical_not(has["south"][side]))
            def _():
                def fill(i, _):
                    buf[(nj + 1) * side, i] = jnp.zeros((nk, nm), jnp.float32)
                    return 0
                lax.fori_loop(0, ni + 2, fill, 0)

            @pl.when(jnp.logical_not(has["east"][side]))
            def _():
                def fill(j, _):
                    buf[j, (ni + 1) * side] = jnp.zeros((nk, nm), jnp.float32)
                    return 0
                lax.fori_loop(1, nj + 1, fill, 0)
    for side in (0, 1):
        @pl.when(jnp.logical_not(has["down"][side]))
        def _():
            def fill(i, _):
                for t in range(STEPS):
                    zrecv[t, side, i] = jnp.zeros((nj, nm), jnp.float32)
                return 0
            lax.fori_loop(0, ni, fill, 0)

    loads[0].wait()

    def pack(i, _):
        for j in range(nj):
            zsend[0, 0, i, j : j + 1] = field[1 + j, 1 + i, 0:1]
            zsend[0, 1, i, j : j + 1] = field[1 + j, 1 + i, nk - 1 : nk]
        return 0

    lax.fori_loop(0, ni, pack, 0)

    def z_start(t, c):
        for side in (1, 0):
            on(has["down"][side], lambda: z_copy(t, side, c).start())

    def send_all_z(c, _):
        z_start(0, c)
        return 0

    lax.fori_loop(0, chunks, send_all_z, 0)
    loads[1].wait()
    loads[2].wait()

    def t_copy(i):
        return remote(total.at[i], below.at[i], tsend_sem.at[i], trecv_sem.at[i], "south", 1)

    first_row = lax.broadcasted_iota(jnp.int32, (8, nm), 0) == 0
    last_row = lax.broadcasted_iota(jnp.int32, (8, nm), 0) == 7

    for t in range(STEPS):
        src, dst = bufs[t % 2], bufs[(t + 1) % 2]
        last = t == STEPS - 1

        def chunk(c, _):
            for side in (0, 1):
                on(has["south"][side], lambda: x_copy(t, 1 - side, c).wait_recv())
                on(has["down"][side], lambda: z_copy(t, 1 - side, c).wait_recv())
            on(jnp.logical_and(has["east"][0], c == 0), lambda: y_copy(t, 1).wait_recv())
            on(jnp.logical_and(has["east"][1], c == chunks - 1), lambda: y_copy(t, 0).wait_recv())
            if t >= 2:
                for side in (0, 1):
                    on(has["south"][side], lambda: x_copy(t - 1, side, c).wait_send())
                on(jnp.logical_and(has["east"][0], c == 0), lambda: y_copy(t - 1, 0).wait_send())
                on(jnp.logical_and(has["east"][1], c == chunks - 1), lambda: y_copy(t - 1, 1).wait_send())

            def row(r, _):
                i = c * ROWS + r
                acc = None
                for j in range(nj):
                    mid = src[1 + j, 1 + i]
                    above = pltpu.roll(mid, 1, 0)
                    under = pltpu.roll(mid, nk - 1, 0)
                    zl = zrecv[t, 0, i, j : j + 1]
                    zh = zrecv[t, 1, i, j : j + 1]
                    above = jnp.concatenate([jnp.where(first_row, zl, above[:8]), above[8:]], axis=0)
                    under = jnp.concatenate([under[:-8], jnp.where(last_row, zh, under[-8:])], axis=0)
                    spread = src[j, 1 + i] + src[2 + j, 1 + i] + src[1 + j, i] + src[1 + j, 2 + i] + above + under - 6.0 * mid
                    new = 2.0 * mid - dst[1 + j, 1 + i] + speed[j, i] * spread
                    dst[1 + j, 1 + i] = new
                    if last:
                        acc = new if acc is None else acc + new
                    else:
                        zsend[t + 1, 0, i, j : j + 1] = new[0:1]
                        zsend[t + 1, 1, i, j : j + 1] = new[nk - 1 : nk]
                if last:
                    total[i] = acc
                return 0

            lax.fori_loop(0, ROWS, row, 0)
            if not last:
                for side in (1, 0):
                    on(has["south"][side], lambda: x_copy(t + 1, side, c).start())
                z_start(t + 1, c)
                on(jnp.logical_and(has["east"][0], c == 0), lambda: y_copy(t + 1, 0).start())
                on(jnp.logical_and(has["east"][1], c == chunks - 1), lambda: y_copy(t + 1, 1).start())
            else:
                def send_row(r, _):
                    t_copy(c * ROWS + r).start()
                    return 0

                @pl.when(jnp.logical_not(has["south"][0]))
                def _():
                    lax.fori_loop(0, ROWS, send_row, 0)
            return 0

        lax.fori_loop(0, chunks, chunk, 0)

    @pl.when(has["south"][0])
    def _():
        def relay(i, _):
            t_copy(i).wait_recv()
            total[i] = total[i] + below[i]
            on(has["south"][1], lambda: t_copy(i).start())
            return 0

        lax.fori_loop(0, ni, relay, 0)

    @pl.when(jnp.logical_not(has["south"][0]))
    def _():
        def fill(i, _):
            below[i] = jnp.zeros((nk, nm), jnp.float32)
            return 0

        lax.fori_loop(0, ni, fill, 0)

    @pl.when(has["south"][1])
    def _():
        def sent(i, _):
            t_copy(i).wait_send()
            return 0

        lax.fori_loop(0, ni, sent, 0)

    def drain(c, _):
        for t in range(STEPS):
            for side in (0, 1):
                if t in (0, STEPS - 1):
                    on(has["south"][side], lambda: x_copy(t, side, c).wait_send())
                on(has["down"][side], lambda: z_copy(t, side, c).wait_send())
        return 0

    lax.fori_loop(0, chunks, drain, 0)
    for t in (0, STEPS - 1):
        for side in (0, 1):
            on(has["east"][side], lambda: y_copy(t, side).wait_send())


def outputs_kernel(grid_j, field, below, running, end, stage, out_sem, field_sem):
    nj, ni, nk, nm = end.shape
    rows = 2
    groups = ni // rows
    whole = pltpu.make_async_copy(field.at[pl.ds(1, nj), pl.ds(1, ni)], end, field_sem)
    whole.start()

    def out(g):
        at = pl.ds(g * rows, rows)
        return pltpu.make_async_copy(stage.at[:, at], running.at[:, at], out_sem.at[g])

    def group(g, _):
        for r in range(rows):
            i = g * rows + r
            acc = below[i]
            for j in range(nj):
                acc = acc + field[1 + j, 1 + i]
                stage[j, i] = acc * (1.0 / grid_j)
        out(g).start()
        return 0

    lax.fori_loop(0, groups, group, 0)

    def done(g, _):
        out(g).wait()
        return 0

    lax.fori_loop(0, groups, done, 0)
    whole.wait()


def shards(field_now, earlier, speed_square):
    shape = field_now.shape
    nj, ni, nk, nm = shape
    padded = (nj + 2, ni + 2, nk, nm)
    chunks = ni // ROWS
    grid_j = nj * lax.axis_size("south")
    dma = pltpu.SemaphoreType.DMA
    anyspace = pl.BlockSpec(memory_space=pltpu.HBM)
    vmem = pl.BlockSpec(memory_space=pltpu.VMEM)
    f32 = jnp.float32
    field, below = pl.pallas_call(
        functools.partial(steps_kernel, grid_j),
        out_shape=(pltpu.VMEM(padded, f32), pltpu.VMEM((ni, nk, nm), f32)),
        in_specs=[anyspace] * 3,
        out_specs=(vmem, vmem),
        scratch_shapes=[
            pltpu.VMEM(padded, f32),
            pltpu.VMEM(shape, f32),
            pltpu.VMEM((STEPS, 2, ni, nj, nm), f32),
            pltpu.VMEM((STEPS, 2, ni, nj, nm), f32),
            pltpu.VMEM((ni, nk, nm), f32),
            dma((3,)),
            dma((STEPS, 2, chunks)), dma((STEPS, 2, chunks)),
            dma((STEPS, 2)), dma((STEPS, 2)),
            dma((STEPS, 2, chunks)), dma((STEPS, 2, chunks)),
            dma((ni,)), dma((ni,)),
        ],
        compiler_params=pltpu.CompilerParams(
            collective_id=0, has_side_effects=True, vmem_limit_bytes=36 * 1024 * 1024,
        ),
        name="steps",
    )(field_now, earlier, speed_square)
    return pl.pallas_call(
        functools.partial(outputs_kernel, grid_j),
        out_shape=(jax.ShapeDtypeStruct(shape, f32), jax.ShapeDtypeStruct(shape, f32)),
        in_specs=[vmem, vmem],
        out_specs=(anyspace, anyspace),
        scratch_shapes=[pltpu.VMEM(shape, f32), dma((ni // 2,)), dma],
        compiler_params=pltpu.CompilerParams(vmem_limit_bytes=32 * 1024 * 1024),
        name="outputs",
    )(field, below)


def solution(mesh):
    placed = P(*AXES, None)
    return jax.shard_map(
        shards,
        mesh=mesh,
        in_specs=(placed, placed, placed),
        out_specs=(placed, placed),
        check_vma=False,
    )
```

```python
import functools

import jax
import jax.numpy as jnp
from jax import lax
from jax.experimental import pallas as pl
from jax.experimental.pallas import tpu as pltpu
from jax.sharding import PartitionSpec as P

STEPS = 4
ROWS = 4
AXES = ("south", "east", "down")
WAYS = {"G": (0,), "H": (1,), "A": (2,), "B": (3,)}


def steps_kernel(
    grid_j, u0, e0, s0, field, below, prev, speed, zsend, zrecv, total, alow, ahigh, slow, shigh,
    load_sem, xsend_sem, xrecv_sem, ysend_sem, yrecv_sem, zsend_sem, zrecv_sem, upsend_sem, uprecv_sem, downsend_sem, downrecv_sem,
):
    nj, ni, nk, nm = s0.shape
    chunks = ni // ROWS
    place = {a: lax.axis_index(a) for a in AXES}
    count = {a: lax.axis_size(a) for a in AXES}
    has = {a: (place[a] > 0, place[a] < count[a] - 1) for a in AXES}
    peer = {a: (place[a] - 1, place[a] + 1) for a in AXES}

    inner = (pl.ds(1, nj), pl.ds(1, ni))
    loads = [
        pltpu.make_async_copy(u0, field.at[inner], load_sem.at[0]),
        pltpu.make_async_copy(e0, prev.at[inner], load_sem.at[1]),
        pltpu.make_async_copy(s0, speed, load_sem.at[2]),
    ]
    for load in loads:
        load.start()

    barrier = pltpu.get_barrier_semaphore()
    greeted = 2
    ring = (lax.rem(place["south"] + count["south"] - 1, count["south"]), lax.rem(place["south"] + 1, count["south"]))
    for side in (0, 1):
        pl.semaphore_signal(barrier, inc=1, device_id={"south": ring[side]}, device_id_type=pl.DeviceIdType.MESH)
    for a in AXES[1:]:
        for side in (0, 1):
            @pl.when(has[a][side])
            def _():
                pl.semaphore_signal(barrier, inc=1, device_id={a: peer[a][side]}, device_id_type=pl.DeviceIdType.MESH)
            greeted = greeted + has[a][side].astype(jnp.int32)
    pl.semaphore_wait(barrier, greeted)

    bufs = (field, prev)

    def remote(src, dst, send_sem, recv_sem, axis, side):
        return pltpu.make_async_remote_copy(
            src_ref=src, dst_ref=dst, send_sem=send_sem, recv_sem=recv_sem,
            device_id={axis: peer[axis][side]}, device_id_type=pl.DeviceIdType.MESH,
        )

    def x_copy(t, side, c, src=None):
        buf = bufs[t % 2]
        rows = pl.ds(1 + c * ROWS, ROWS)
        own, dst = (nj if side else 1), (0 if side else nj + 1)
        src = buf.at[own, rows] if src is None else src
        return remote(src, buf.at[dst, rows], xsend_sem.at[t, side, c], xrecv_sem.at[t, 1 - side, c], "south", side)

    def y_copy(t, side, src=None):
        buf = bufs[t % 2]
        own, dst = (ni if side else 1), (0 if side else ni + 1)
        src = buf.at[pl.ds(1, nj), own] if src is None else src
        return remote(src, buf.at[pl.ds(1, nj), dst], ysend_sem.at[t, side], yrecv_sem.at[t, 1 - side], "east", side)

    def z_copy(t, side, c):
        rows = pl.ds(c * ROWS, ROWS)
        return remote(
            zsend.at[t, side, rows], zrecv.at[t, 1 - side, rows],
            zsend_sem.at[t, side, c], zrecv_sem.at[t, 1 - side, c], "down", side,
        )

    def on(pred, action):
        @pl.when(pred)
        def _():
            action()

    for c in range(chunks):
        rows = pl.ds(c * ROWS, ROWS)
        for side in (1, 0):
            on(has["south"][side], lambda: x_copy(0, side, c, u0.at[nj - 1 if side else 0, rows]).start())
    for side in (1, 0):
        on(has["east"][side], lambda: y_copy(0, side, u0.at[:, ni - 1 if side else 0]).start())

    for buf in bufs:
        for side in (0, 1):
            @pl.when(jnp.logical_not(has["south"][side]))
            def _():
                def fill(i, _):
                    buf[(nj + 1) * side, i] = jnp.zeros((nk, nm), jnp.float32)
                    return 0
                lax.fori_loop(0, ni + 2, fill, 0)

            @pl.when(jnp.logical_not(has["east"][side]))
            def _():
                def fill(j, _):
                    buf[j, (ni + 1) * side] = jnp.zeros((nk, nm), jnp.float32)
                    return 0
                lax.fori_loop(1, nj + 1, fill, 0)
    for side in (0, 1):
        @pl.when(jnp.logical_not(has["down"][side]))
        def _():
            def fill(i, _):
                for t in range(STEPS):
                    zrecv[t, side, i] = jnp.zeros((nj, nm), jnp.float32)
                return 0
            lax.fori_loop(0, ni, fill, 0)

    loads[0].wait()

    def pack(i, _):
        for j in range(nj):
            zsend[0, 0, i, j : j + 1] = field[1 + j, 1 + i, 0:1]
            zsend[0, 1, i, j : j + 1] = field[1 + j, 1 + i, nk - 1 : nk]
        return 0

    lax.fori_loop(0, ni, pack, 0)

    def z_start(t, c):
        for side in (1, 0):
            on(has["down"][side], lambda: z_copy(t, side, c).start())

    def send_all_z(c, _):
        z_start(0, c)
        return 0

    lax.fori_loop(0, chunks, send_all_z, 0)
    loads[1].wait()
    loads[2].wait()

    def up(src, dst, i):
        return pltpu.make_async_remote_copy(
            src_ref=src.at[i], dst_ref=dst.at[i], send_sem=upsend_sem.at[i], recv_sem=uprecv_sem.at[i],
            device_id={"south": ring[1]}, device_id_type=pl.DeviceIdType.MESH,
        )

    def down(src, dst, i):
        return pltpu.make_async_remote_copy(
            src_ref=src.at[i], dst_ref=dst.at[i], send_sem=downsend_sem.at[i], recv_sem=downrecv_sem.at[i],
            device_id={"south": ring[0]}, device_id_type=pl.DeviceIdType.MESH,
        )

    ways = {w: [c * ROWS + r for c in cs for r in range(ROWS)] for w, cs in WAYS.items()}
    first = {
        0: (("G", down, ahigh), ("A", up, below), ("B", up, below), ("H", up, below)),
        1: (("G", up, alow), ("H", down, ahigh)),
        2: (("H", up, alow), ("B", down, ahigh)),
        3: (),
    }

    def send_totals(c):
        for x, sends in first.items():
            ready = []
            latest = {"up": 0, "down": 0}
            for w, go, target in sends:
                key = "up" if go is up else "down"
                latest[key] = max(latest[key], max(WAYS[w]))
                if latest[key] == c:
                    ready.append((w, go, target))
            if ready:
                @pl.when(place["south"] == x)
                def _():
                    for w, go, target in ready:
                        for i in ways[w]:
                            go(total, target, i).start()

    first_row = lax.broadcasted_iota(jnp.int32, (8, nm), 0) == 0
    last_row = lax.broadcasted_iota(jnp.int32, (8, nm), 0) == 7

    for t in range(STEPS):
        src, dst = bufs[t % 2], bufs[(t + 1) % 2]
        last = t == STEPS - 1

        def chunk(c, _, t=t, src=src, dst=dst, last=last):
            for side in (0, 1):
                on(has["south"][side], lambda: x_copy(t, 1 - side, c).wait_recv())
                on(has["down"][side], lambda: z_copy(t, 1 - side, c).wait_recv())
            on(jnp.logical_and(has["east"][0], c == 0), lambda: y_copy(t, 1).wait_recv())
            on(jnp.logical_and(has["east"][1], c == chunks - 1), lambda: y_copy(t, 0).wait_recv())
            if t >= 2:
                for side in (0, 1):
                    on(has["south"][side], lambda: x_copy(t - 1, side, c).wait_send())
                on(jnp.logical_and(has["east"][0], c == 0), lambda: y_copy(t - 1, 0).wait_send())
                on(jnp.logical_and(has["east"][1], c == chunks - 1), lambda: y_copy(t - 1, 1).wait_send())

            def row(r, _):
                i = c * ROWS + r
                acc = None
                for j in range(nj):
                    mid = src[1 + j, 1 + i]
                    above = pltpu.roll(mid, 1, 0)
                    under = pltpu.roll(mid, nk - 1, 0)
                    zl = zrecv[t, 0, i, j : j + 1]
                    zh = zrecv[t, 1, i, j : j + 1]
                    above = jnp.concatenate([jnp.where(first_row, zl, above[:8]), above[8:]], axis=0)
                    under = jnp.concatenate([under[:-8], jnp.where(last_row, zh, under[-8:])], axis=0)
                    spread = src[j, 1 + i] + src[2 + j, 1 + i] + src[1 + j, i] + src[1 + j, 2 + i] + above + under - 6.0 * mid
                    new = 2.0 * mid - dst[1 + j, 1 + i] + speed[j, i] * spread
                    dst[1 + j, 1 + i] = new
                    if last:
                        acc = new if acc is None else acc + new
                    else:
                        zsend[t + 1, 0, i, j : j + 1] = new[0:1]
                        zsend[t + 1, 1, i, j : j + 1] = new[nk - 1 : nk]
                if last:
                    total[i] = acc
                return 0

            lax.fori_loop(0, ROWS, row, 0)
            if not last:
                for side in (1, 0):
                    on(has["south"][side], lambda: x_copy(t + 1, side, c).start())
                z_start(t + 1, c)
                on(jnp.logical_and(has["east"][0], c == 0), lambda: y_copy(t + 1, 0).start())
                on(jnp.logical_and(has["east"][1], c == chunks - 1), lambda: y_copy(t + 1, 1).start())
            return 0

        if last:
            for c in range(chunks):
                chunk(c, 0)
                send_totals(c)
        else:
            lax.fori_loop(0, chunks, chunk, 0)

    def got_up(i):
        up(total, below, i).wait_recv()

    def got_down(i):
        down(total, below, i).wait_recv()

    def pairs(a, b):
        for k in range(max(len(ways[a]), len(ways[b]))):
            yield ways[a][k] if k < len(ways[a]) else None, ways[b][k] if k < len(ways[b]) else None

    @pl.when(place["south"] == 0)
    def _():
        for w, target in (("H", ahigh), ("B", below)):
            for i in ways[w]:
                got_down(i)
                shigh[i] = total[i] + ahigh[i]
                down(shigh, target, i).start()
        for i in range(ni):
            below[i] = jnp.zeros((nk, nm), jnp.float32)
        for w in "ABH":
            for i in ways[w]:
                up(total, below, i).wait_send()
        for w in "GHB":
            for i in ways[w]:
                down(total, below, i).wait_send()

    @pl.when(place["south"] == 1)
    def _():
        def relay_up(i):
            got_up(i)
            slow[i] = below[i] + total[i]
            up(slow, below, i).start()

        for a, b in pairs("A", "B"):
            if a is not None:
                relay_up(a)
            if b is not None:
                got_down(b)
                shigh[b] = total[b] + ahigh[b]
                down(shigh, ahigh, b).start()
        for i in ways["B"]:
            relay_up(i)
        for i in ways["G"]:
            got_down(i)
        for i in ways["H"]:
            got_up(i)
        for w in "GAB":
            for i in ways[w]:
                up(total, below, i).wait_send()
        for w in "HB":
            for i in ways[w]:
                down(total, below, i).wait_send()

    @pl.when(place["south"] == 2)
    def _():
        for i in ways["G"]:
            got_up(i)
            slow[i] = alow[i] + total[i]
            up(slow, alow, i).start()
        for g, a in pairs("G", "A"):
            if g is not None:
                got_down(g)
                down(ahigh, below, g).start()
                below[g] = ahigh[g] + alow[g]
            if a is not None:
                got_up(a)
                slow[a] = below[a] + total[a]
                up(slow, below, a).start()
        for i in ways["B"]:
            got_up(i)
        for i in ways["H"]:
            got_down(i)
        for w in "HGA":
            for i in ways[w]:
                up(total, below, i).wait_send()
        for w in "BG":
            for i in ways[w]:
                down(total, below, i).wait_send()

    @pl.when(place["south"] == 3)
    def _():
        for i in ways["G"]:
            got_down(i)
            down(ahigh, ahigh, i).start()
        for i in ways["H"]:
            got_down(i)
            down(ahigh, below, i).start()
            got_up(i)
            below[i] = ahigh[i] + alow[i]
        for i in ways["G"]:
            got_up(i)
            below[i] = ahigh[i] + alow[i]
        for i in ways["A"]:
            got_up(i)
        for i in ways["B"]:
            got_down(i)
        for w in "GH":
            for i in ways[w]:
                down(total, below, i).wait_send()

    def drain(c, _):
        for t in range(STEPS):
            for side in (0, 1):
                if t in (0, STEPS - 1):
                    on(has["south"][side], lambda: x_copy(t, side, c).wait_send())
                on(has["down"][side], lambda: z_copy(t, side, c).wait_send())
        return 0

    lax.fori_loop(0, chunks, drain, 0)
    for t in (0, STEPS - 1):
        for side in (0, 1):
            on(has["east"][side], lambda: y_copy(t, side).wait_send())


def outputs_kernel(grid_j, field, below, running, end, stage, out_sem, field_sem):
    nj, ni, nk, nm = end.shape
    rows = 2
    groups = ni // rows
    whole = pltpu.make_async_copy(field.at[pl.ds(1, nj), pl.ds(1, ni)], end, field_sem)
    whole.start()

    def out(g):
        at = pl.ds(g * rows, rows)
        return pltpu.make_async_copy(stage.at[:, at], running.at[:, at], out_sem.at[g])

    def group(g, _):
        for r in range(rows):
            i = g * rows + r
            acc = below[i]
            for j in range(nj):
                acc = acc + field[1 + j, 1 + i]
                stage[j, i] = acc * (1.0 / grid_j)
        out(g).start()
        return 0

    lax.fori_loop(0, groups, group, 0)

    def done(g, _):
        out(g).wait()
        return 0

    lax.fori_loop(0, groups, done, 0)
    whole.wait()


def shards(field_now, earlier, speed_square):
    shape = field_now.shape
    nj, ni, nk, nm = shape
    padded = (nj + 2, ni + 2, nk, nm)
    chunks = ni // ROWS
    grid_j = nj * lax.axis_size("south")
    dma = pltpu.SemaphoreType.DMA
    anyspace = pl.BlockSpec(memory_space=pltpu.HBM)
    vmem = pl.BlockSpec(memory_space=pltpu.VMEM)
    f32 = jnp.float32
    field, below = pl.pallas_call(
        functools.partial(steps_kernel, grid_j),
        out_shape=(pltpu.VMEM(padded, f32), pltpu.VMEM((ni, nk, nm), f32)),
        in_specs=[anyspace] * 3,
        out_specs=(vmem, vmem),
        scratch_shapes=[
            pltpu.VMEM(padded, f32),
            pltpu.VMEM(shape, f32),
            pltpu.VMEM((STEPS, 2, ni, nj, nm), f32),
            pltpu.VMEM((STEPS, 2, ni, nj, nm), f32),
            *[pltpu.VMEM((ni, nk, nm), f32)] * 5,
            dma((3,)),
            dma((STEPS, 2, chunks)), dma((STEPS, 2, chunks)),
            dma((STEPS, 2)), dma((STEPS, 2)),
            dma((STEPS, 2, chunks)), dma((STEPS, 2, chunks)),
            *[dma((ni,))] * 4,
        ],
        compiler_params=pltpu.CompilerParams(
            collective_id=0, has_side_effects=True, vmem_limit_bytes=40 * 1024 * 1024,
        ),
        name="steps",
    )(field_now, earlier, speed_square)
    return pl.pallas_call(
        functools.partial(outputs_kernel, grid_j),
        out_shape=(jax.ShapeDtypeStruct(shape, f32), jax.ShapeDtypeStruct(shape, f32)),
        in_specs=[vmem, vmem],
        out_specs=(anyspace, anyspace),
        scratch_shapes=[pltpu.VMEM(shape, f32), dma((ni // 2,)), dma],
        compiler_params=pltpu.CompilerParams(vmem_limit_bytes=32 * 1024 * 1024),
        name="outputs",
    )(field, below)


def solution(mesh):
    placed = P(*AXES, None)
    return jax.shard_map(
        shards,
        mesh=mesh,
        in_specs=(placed, placed, placed),
        out_specs=(placed, placed),
        check_vma=False,
    )
```

```python
import functools

import jax
import jax.numpy as jnp
from jax import lax
from jax.experimental import pallas as pl
from jax.experimental.pallas import tpu as pltpu
from jax.sharding import PartitionSpec as P

STEPS = 4
ROWS = 4
AXES = ("south", "east", "down")
WAYS = {"G": (0,), "H": (1,), "A": (2,), "B": (3,)}


def steps_kernel(
    grid_j, u0, e0, s0, field, below, prev, speed, zsend, zrecv, total, alow, ahigh, slow, shigh, lead,
    load_sem, xsend_sem, xrecv_sem, ysend_sem, yrecv_sem, zsend_sem, zrecv_sem, upsend_sem, uprecv_sem, downsend_sem, downrecv_sem,
):
    nj, ni, nk, nm = s0.shape
    chunks = ni // ROWS
    place = {a: lax.axis_index(a) for a in AXES}
    count = {a: lax.axis_size(a) for a in AXES}
    has = {a: (place[a] > 0, place[a] < count[a] - 1) for a in AXES}
    peer = {a: (place[a] - 1, place[a] + 1) for a in AXES}

    barrier = pltpu.get_barrier_semaphore()
    greeted = 0
    for a in AXES:
        for side in (0, 1):
            @pl.when(has[a][side])
            def _():
                pl.semaphore_signal(barrier, inc=1, device_id={a: peer[a][side]}, device_id_type=pl.DeviceIdType.MESH)
            greeted = greeted + has[a][side].astype(jnp.int32)

    inner = (pl.ds(1, nj), pl.ds(1, ni))
    leads = [
        pltpu.make_async_copy(u0.at[(nj - 1) * side, pl.ds(0, ROWS)], lead.at[side], load_sem.at[3 + side]) for side in (0, 1)
    ]
    loads = [
        pltpu.make_async_copy(u0, field.at[inner], load_sem.at[0]),
        pltpu.make_async_copy(e0, prev.at[inner], load_sem.at[1]),
        pltpu.make_async_copy(s0, speed, load_sem.at[2]),
    ]
    for load in leads + loads:
        load.start()
    ring = (lax.rem(place["south"] + count["south"] - 1, count["south"]), lax.rem(place["south"] + 1, count["south"]))
    for load in leads:
        load.wait()
    pl.semaphore_wait(barrier, greeted)

    bufs = (field, prev)

    def remote(src, dst, send_sem, recv_sem, axis, side):
        return pltpu.make_async_remote_copy(
            src_ref=src, dst_ref=dst, send_sem=send_sem, recv_sem=recv_sem,
            device_id={axis: peer[axis][side]}, device_id_type=pl.DeviceIdType.MESH,
        )

    def x_copy(t, side, c, src=None):
        buf = bufs[t % 2]
        rows = pl.ds(1 + c * ROWS, ROWS)
        own, dst = (nj if side else 1), (0 if side else nj + 1)
        src = buf.at[own, rows] if src is None else src
        return remote(src, buf.at[dst, rows], xsend_sem.at[t, side, c], xrecv_sem.at[t, 1 - side, c], "south", side)

    def y_copy(t, side, src=None):
        buf = bufs[t % 2]
        own, dst = (ni if side else 1), (0 if side else ni + 1)
        src = buf.at[pl.ds(1, nj), own] if src is None else src
        return remote(src, buf.at[pl.ds(1, nj), dst], ysend_sem.at[t, side], yrecv_sem.at[t, 1 - side], "east", side)

    def z_copy(t, side, c):
        rows = pl.ds(c * ROWS, ROWS)
        return remote(
            zsend.at[t, side, rows], zrecv.at[t, 1 - side, rows],
            zsend_sem.at[t, side, c], zrecv_sem.at[t, 1 - side, c], "down", side,
        )

    def on(pred, action):
        @pl.when(pred)
        def _():
            action()

    for c in range(chunks):
        rows = pl.ds(c * ROWS, ROWS)
        for side in (1, 0):
            face = u0.at[nj - 1 if side else 0, rows] if c else lead.at[side]
            on(has["south"][side], lambda: x_copy(0, side, c, face).start())
    for side in (1, 0):
        on(has["east"][side], lambda: y_copy(0, side, u0.at[:, ni - 1 if side else 0]).start())

    for buf in bufs:
        for side in (0, 1):
            @pl.when(jnp.logical_not(has["south"][side]))
            def _():
                def fill(i, _):
                    buf[(nj + 1) * side, i] = jnp.zeros((nk, nm), jnp.float32)
                    return 0
                lax.fori_loop(0, ni + 2, fill, 0)

            @pl.when(jnp.logical_not(has["east"][side]))
            def _():
                def fill(j, _):
                    buf[j, (ni + 1) * side] = jnp.zeros((nk, nm), jnp.float32)
                    return 0
                lax.fori_loop(1, nj + 1, fill, 0)
    for side in (0, 1):
        @pl.when(jnp.logical_not(has["down"][side]))
        def _():
            def fill(i, _):
                for t in range(STEPS):
                    zrecv[t, side, i] = jnp.zeros((nj, nm), jnp.float32)
                return 0
            lax.fori_loop(0, ni, fill, 0)

    loads[0].wait()

    def pack(i, _):
        for j in range(nj):
            zsend[0, 0, i, j : j + 1] = field[1 + j, 1 + i, 0:1]
            zsend[0, 1, i, j : j + 1] = field[1 + j, 1 + i, nk - 1 : nk]
        return 0

    lax.fori_loop(0, ni, pack, 0)

    def z_start(t, c):
        for side in (1, 0):
            on(has["down"][side], lambda: z_copy(t, side, c).start())

    def send_all_z(c, _):
        z_start(0, c)
        return 0

    lax.fori_loop(0, chunks, send_all_z, 0)
    loads[1].wait()
    loads[2].wait()

    def up(src, dst, i):
        return pltpu.make_async_remote_copy(
            src_ref=src.at[i], dst_ref=dst.at[i], send_sem=upsend_sem.at[i], recv_sem=uprecv_sem.at[i],
            device_id={"south": ring[1]}, device_id_type=pl.DeviceIdType.MESH,
        )

    def down(src, dst, i):
        return pltpu.make_async_remote_copy(
            src_ref=src.at[i], dst_ref=dst.at[i], send_sem=downsend_sem.at[i], recv_sem=downrecv_sem.at[i],
            device_id={"south": ring[0]}, device_id_type=pl.DeviceIdType.MESH,
        )

    ways = {w: [c * ROWS + r for c in cs for r in range(ROWS)] for w, cs in WAYS.items()}
    first = {
        0: (("G", down, ahigh), ("A", up, below), ("B", up, below), ("H", up, below)),
        1: (("G", up, alow), ("H", down, ahigh)),
        2: (("H", up, alow), ("B", down, ahigh)),
        3: (),
    }

    def send_totals(c):
        for x, sends in first.items():
            ready = []
            latest = {"up": 0, "down": 0}
            for w, go, target in sends:
                key = "up" if go is up else "down"
                latest[key] = max(latest[key], max(WAYS[w]))
                if latest[key] == c:
                    ready.append((w, go, target))
            if ready:
                @pl.when(place["south"] == x)
                def _():
                    for w, go, target in ready:
                        for i in ways[w]:
                            go(total, target, i).start()

    first_row = lax.broadcasted_iota(jnp.int32, (8, nm), 0) == 0
    last_row = lax.broadcasted_iota(jnp.int32, (8, nm), 0) == 7

    for t in range(STEPS):
        src, dst = bufs[t % 2], bufs[(t + 1) % 2]
        last = t == STEPS - 1

        def chunk(c, _, t=t, src=src, dst=dst, last=last):
            for side in (0, 1):
                on(has["south"][side], lambda: x_copy(t, 1 - side, c).wait_recv())
                on(has["down"][side], lambda: z_copy(t, 1 - side, c).wait_recv())
            on(jnp.logical_and(has["east"][0], c == 0), lambda: y_copy(t, 1).wait_recv())
            on(jnp.logical_and(has["east"][1], c == chunks - 1), lambda: y_copy(t, 0).wait_recv())
            if t >= 2:
                for side in (0, 1):
                    on(has["south"][side], lambda: x_copy(t - 1, side, c).wait_send())
                on(jnp.logical_and(has["east"][0], c == 0), lambda: y_copy(t - 1, 0).wait_send())
                on(jnp.logical_and(has["east"][1], c == chunks - 1), lambda: y_copy(t - 1, 1).wait_send())

            def row(r, _):
                i = c * ROWS + r
                acc = None
                for j in range(nj):
                    mid = src[1 + j, 1 + i]
                    above = pltpu.roll(mid, 1, 0)
                    under = pltpu.roll(mid, nk - 1, 0)
                    zl = zrecv[t, 0, i, j : j + 1]
                    zh = zrecv[t, 1, i, j : j + 1]
                    above = jnp.concatenate([jnp.where(first_row, zl, above[:8]), above[8:]], axis=0)
                    under = jnp.concatenate([under[:-8], jnp.where(last_row, zh, under[-8:])], axis=0)
                    spread = src[j, 1 + i] + src[2 + j, 1 + i] + src[1 + j, i] + src[1 + j, 2 + i] + above + under - 6.0 * mid
                    new = 2.0 * mid - dst[1 + j, 1 + i] + speed[j, i] * spread
                    dst[1 + j, 1 + i] = new
                    if last:
                        acc = new if acc is None else acc + new
                    else:
                        zsend[t + 1, 0, i, j : j + 1] = new[0:1]
                        zsend[t + 1, 1, i, j : j + 1] = new[nk - 1 : nk]
                if last:
                    total[i] = acc
                return 0

            lax.fori_loop(0, ROWS, row, 0)
            if not last:
                for side in (1, 0):
                    on(has["south"][side], lambda: x_copy(t + 1, side, c).start())
                z_start(t + 1, c)
                on(jnp.logical_and(has["east"][0], c == 0), lambda: y_copy(t + 1, 0).start())
                on(jnp.logical_and(has["east"][1], c == chunks - 1), lambda: y_copy(t + 1, 1).start())
            return 0

        if last:
            for c in range(chunks):
                chunk(c, 0)
                send_totals(c)
        else:
            lax.fori_loop(0, chunks, chunk, 0)

    def got_up(i):
        up(total, below, i).wait_recv()

    def got_down(i):
        down(total, below, i).wait_recv()

    def pairs(a, b):
        for k in range(max(len(ways[a]), len(ways[b]))):
            yield ways[a][k] if k < len(ways[a]) else None, ways[b][k] if k < len(ways[b]) else None

    @pl.when(place["south"] == 0)
    def _():
        for w, target in (("H", ahigh), ("B", below)):
            for i in ways[w]:
                got_down(i)
                shigh[i] = total[i] + ahigh[i]
                down(shigh, target, i).start()
        for i in range(ni):
            below[i] = jnp.zeros((nk, nm), jnp.float32)
        for w in "ABH":
            for i in ways[w]:
                up(total, below, i).wait_send()
        for w in "GHB":
            for i in ways[w]:
                down(total, below, i).wait_send()

    @pl.when(place["south"] == 1)
    def _():
        def relay_up(i):
            got_up(i)
            slow[i] = below[i] + total[i]
            up(slow, below, i).start()

        for a, b in pairs("A", "B"):
            if a is not None:
                relay_up(a)
            if b is not None:
                got_down(b)
                shigh[b] = total[b] + ahigh[b]
                down(shigh, ahigh, b).start()
        for i in ways["B"]:
            relay_up(i)
        for i in ways["G"]:
            got_down(i)
        for i in ways["H"]:
            got_up(i)
        for w in "GAB":
            for i in ways[w]:
                up(total, below, i).wait_send()
        for w in "HB":
            for i in ways[w]:
                down(total, below, i).wait_send()

    @pl.when(place["south"] == 2)
    def _():
        for i in ways["G"]:
            got_up(i)
            slow[i] = alow[i] + total[i]
            up(slow, alow, i).start()
        for g, a in pairs("G", "A"):
            if g is not None:
                got_down(g)
                down(ahigh, below, g).start()
                below[g] = ahigh[g] + alow[g]
            if a is not None:
                got_up(a)
                slow[a] = below[a] + total[a]
                up(slow, below, a).start()
        for i in ways["B"]:
            got_up(i)
        for i in ways["H"]:
            got_down(i)
        for w in "HGA":
            for i in ways[w]:
                up(total, below, i).wait_send()
        for w in "BG":
            for i in ways[w]:
                down(total, below, i).wait_send()

    @pl.when(place["south"] == 3)
    def _():
        for i in ways["G"]:
            got_down(i)
            down(ahigh, ahigh, i).start()
        for i in ways["H"]:
            got_down(i)
            down(ahigh, below, i).start()
            got_up(i)
            below[i] = ahigh[i] + alow[i]
        for i in ways["G"]:
            got_up(i)
            below[i] = ahigh[i] + alow[i]
        for i in ways["A"]:
            got_up(i)
        for i in ways["B"]:
            got_down(i)
        for w in "GH":
            for i in ways[w]:
                down(total, below, i).wait_send()

    def drain(c, _):
        for t in range(STEPS):
            for side in (0, 1):
                if t in (0, STEPS - 1):
                    on(has["south"][side], lambda: x_copy(t, side, c).wait_send())
                on(has["down"][side], lambda: z_copy(t, side, c).wait_send())
        return 0

    lax.fori_loop(0, chunks, drain, 0)
    for t in (0, STEPS - 1):
        for side in (0, 1):
            on(has["east"][side], lambda: y_copy(t, side).wait_send())


def outputs_kernel(grid_j, field, below, running, end, stage, out_sem, field_sem):
    nj, ni, nk, nm = end.shape
    rows = 2
    groups = ni // rows
    whole = pltpu.make_async_copy(field.at[pl.ds(1, nj), pl.ds(1, ni)], end, field_sem)
    whole.start()

    def out(g):
        at = pl.ds(g * rows, rows)
        return pltpu.make_async_copy(stage.at[:, at], running.at[:, at], out_sem.at[g])

    def group(g, _):
        for r in range(rows):
            i = g * rows + r
            acc = below[i]
            for j in range(nj):
                acc = acc + field[1 + j, 1 + i]
                stage[j, i] = acc * (1.0 / grid_j)
        out(g).start()
        return 0

    lax.fori_loop(0, groups, group, 0)

    def done(g, _):
        out(g).wait()
        return 0

    lax.fori_loop(0, groups, done, 0)
    whole.wait()


def shards(field_now, earlier, speed_square):
    shape = field_now.shape
    nj, ni, nk, nm = shape
    padded = (nj + 2, ni + 2, nk, nm)
    chunks = ni // ROWS
    grid_j = nj * lax.axis_size("south")
    dma = pltpu.SemaphoreType.DMA
    anyspace = pl.BlockSpec(memory_space=pltpu.HBM)
    vmem = pl.BlockSpec(memory_space=pltpu.VMEM)
    f32 = jnp.float32
    field, below = pl.pallas_call(
        functools.partial(steps_kernel, grid_j),
        out_shape=(pltpu.VMEM(padded, f32), pltpu.VMEM((ni, nk, nm), f32)),
        in_specs=[anyspace] * 3,
        out_specs=(vmem, vmem),
        scratch_shapes=[
            pltpu.VMEM(padded, f32),
            pltpu.VMEM(shape, f32),
            pltpu.VMEM((STEPS, 2, ni, nj, nm), f32),
            pltpu.VMEM((STEPS, 2, ni, nj, nm), f32),
            *[pltpu.VMEM((ni, nk, nm), f32)] * 5,
            pltpu.VMEM((2, ROWS, nk, nm), f32),
            dma((5,)),
            dma((STEPS, 2, chunks)), dma((STEPS, 2, chunks)),
            dma((STEPS, 2)), dma((STEPS, 2)),
            dma((STEPS, 2, chunks)), dma((STEPS, 2, chunks)),
            *[dma((ni,))] * 4,
        ],
        compiler_params=pltpu.CompilerParams(
            collective_id=0, has_side_effects=True, vmem_limit_bytes=40 * 1024 * 1024,
        ),
        name="steps",
    )(field_now, earlier, speed_square)
    return pl.pallas_call(
        functools.partial(outputs_kernel, grid_j),
        out_shape=(jax.ShapeDtypeStruct(shape, f32), jax.ShapeDtypeStruct(shape, f32)),
        in_specs=[vmem, vmem],
        out_specs=(anyspace, anyspace),
        scratch_shapes=[pltpu.VMEM(shape, f32), dma((ni // 2,)), dma],
        compiler_params=pltpu.CompilerParams(vmem_limit_bytes=32 * 1024 * 1024),
        name="outputs",
    )(field, below)


def solution(mesh):
    placed = P(*AXES, None)
    return jax.shard_map(
        shards,
        mesh=mesh,
        in_specs=(placed, placed, placed),
        out_specs=(placed, placed),
        check_vma=False,
    )
```

```python
import functools

import jax
import jax.numpy as jnp
from jax import lax
from jax.experimental import pallas as pl
from jax.experimental.pallas import tpu as pltpu
from jax.sharding import PartitionSpec as P

STEPS = 4
ROWS = 4
AXES = ("south", "east", "down")
WAYS = {"G": (0,), "H": (1,), "A": (2,), "B": (3,)}


def steps_kernel(
    grid_j, u0, e0, s0, field, below, prev, speed, zsend, zrecv, total, alow, ahigh, slow, shigh, lead,
    load_sem, xsend_sem, xrecv_sem, ysend_sem, yrecv_sem, zsend_sem, zrecv_sem, total_sem, uprecv_sem, downrecv_sem,
):
    nj, ni, nk, nm = s0.shape
    chunks = ni // ROWS
    place = {a: lax.axis_index(a) for a in AXES}
    count = {a: lax.axis_size(a) for a in AXES}
    has = {a: (place[a] > 0, place[a] < count[a] - 1) for a in AXES}
    peer = {a: (place[a] - 1, place[a] + 1) for a in AXES}

    barrier = pltpu.get_barrier_semaphore()
    greeted = 0
    for a in AXES:
        for side in (0, 1):
            @pl.when(has[a][side])
            def _():
                pl.semaphore_signal(barrier, inc=1, device_id={a: peer[a][side]}, device_id_type=pl.DeviceIdType.MESH)
            greeted = greeted + has[a][side].astype(jnp.int32)

    inner = (pl.ds(1, nj), pl.ds(1, ni))
    leads = [
        pltpu.make_async_copy(u0.at[(nj - 1) * side, pl.ds(0, ROWS)], lead.at[side], load_sem.at[3]) for side in (0, 1)
    ]
    loads = [
        pltpu.make_async_copy(u0, field.at[inner], load_sem.at[0]),
        pltpu.make_async_copy(e0, prev.at[inner], load_sem.at[1]),
        pltpu.make_async_copy(s0, speed, load_sem.at[2]),
    ]
    for load in leads + loads:
        load.start()
    ring = (lax.rem(place["south"] + count["south"] - 1, count["south"]), lax.rem(place["south"] + 1, count["south"]))
    pltpu.make_async_copy(u0.at[pl.ds(0, 2), pl.ds(0, ROWS)], lead, load_sem.at[3]).wait()
    pl.semaphore_wait(barrier, greeted)

    bufs = (field, prev)

    def remote(src, dst, send_sem, recv_sem, axis, side):
        return pltpu.make_async_remote_copy(
            src_ref=src, dst_ref=dst, send_sem=send_sem, recv_sem=recv_sem,
            device_id={axis: peer[axis][side]}, device_id_type=pl.DeviceIdType.MESH,
        )

    def x_copy(t, side, c, src=None):
        buf = bufs[t % 2]
        rows = pl.ds(1 + c * ROWS, ROWS)
        own, dst = (nj if side else 1), (0 if side else nj + 1)
        src = buf.at[own, rows] if src is None else src
        return remote(src, buf.at[dst, rows], xsend_sem.at[t % 2, side], xrecv_sem.at[t % 2, c], "south", side)

    def y_copy(t, side, src=None):
        buf = bufs[t % 2]
        own, dst = (ni if side else 1), (0 if side else ni + 1)
        src = buf.at[pl.ds(1, nj), own] if src is None else src
        return remote(src, buf.at[pl.ds(1, nj), dst], ysend_sem.at[t % 2, side], yrecv_sem.at[t % 2, 1 - side], "east", side)

    def z_copy(t, side, c):
        rows = pl.ds(c * ROWS, ROWS)
        return remote(
            zsend.at[t, side, rows], zrecv.at[t, 1 - side, rows],
            zsend_sem.at[side], zrecv_sem.at[t % 2, c], "down", side,
        )

    def arrived(axis, sem, one, both):
        two = jnp.logical_and(*has[axis])
        for pred, ref in ((two, both), (jnp.logical_not(two), one)):
            @pl.when(pred)
            def _():
                remote(ref, ref, zsend_sem.at[0], sem, axis, 0).wait_recv()

    def sent(axis, sems, ref):
        for side in (0, 1):
            on(has[axis][side], lambda: remote(ref, ref, sems(side), zrecv_sem.at[0, 0], axis, side).wait_send())

    def sent_faces(t):
        sent("south", lambda side: xsend_sem.at[t % 2, side], field.at[0, pl.ds(1, ni)])
        sent("east", lambda side: ysend_sem.at[t % 2, side], field.at[pl.ds(1, nj), 0])

    def on(pred, action):
        @pl.when(pred)
        def _():
            action()

    for c in range(chunks):
        rows = pl.ds(c * ROWS, ROWS)
        for side in (1, 0):
            face = u0.at[nj - 1 if side else 0, rows] if c else lead.at[side]
            on(has["south"][side], lambda: x_copy(0, side, c, face).start())
    for side in (1, 0):
        on(has["east"][side], lambda: y_copy(0, side, u0.at[:, ni - 1 if side else 0]).start())

    for buf in bufs:
        for side in (0, 1):
            @pl.when(jnp.logical_not(has["south"][side]))
            def _():
                def fill(i, _):
                    buf[(nj + 1) * side, i] = jnp.zeros((nk, nm), jnp.float32)
                    return 0
                lax.fori_loop(0, ni + 2, fill, 0)

            @pl.when(jnp.logical_not(has["east"][side]))
            def _():
                def fill(j, _):
                    buf[j, (ni + 1) * side] = jnp.zeros((nk, nm), jnp.float32)
                    return 0
                lax.fori_loop(1, nj + 1, fill, 0)
    for side in (0, 1):
        @pl.when(jnp.logical_not(has["down"][side]))
        def _():
            def fill(i, _):
                for t in range(STEPS):
                    zrecv[t, side, i] = jnp.zeros((nj, nm), jnp.float32)
                return 0
            lax.fori_loop(0, ni, fill, 0)

    loads[0].wait()

    def pack(i, _):
        for j in range(nj):
            zsend[0, 0, i, j : j + 1] = field[1 + j, 1 + i, 0:1]
            zsend[0, 1, i, j : j + 1] = field[1 + j, 1 + i, nk - 1 : nk]
        return 0

    lax.fori_loop(0, ni, pack, 0)

    def z_start(t, c):
        for side in (1, 0):
            on(has["down"][side], lambda: z_copy(t, side, c).start())

    def send_all_z(c, _):
        z_start(0, c)
        return 0

    lax.fori_loop(0, chunks, send_all_z, 0)
    loads[1].wait()
    loads[2].wait()

    ways = {w: [c * ROWS + r for c in cs for r in range(ROWS)] for w, cs in WAYS.items()}
    came = {"up": {1: "ABH", 2: "GAB", 3: "HGA"}, "down": {0: "HB", 1: "BG", 2: "GH", 3: "GHB"}}
    slot = {(key, x): [i for w in ws for i in ways[w]].index for key, at in came.items() for x, ws in at.items()}

    def up(src, dst, i, x):
        return pltpu.make_async_remote_copy(
            src_ref=src.at[i], dst_ref=dst.at[i], send_sem=total_sem.at[0], recv_sem=uprecv_sem.at[slot["up", x + 1](i)],
            device_id={"south": ring[1]}, device_id_type=pl.DeviceIdType.MESH,
        )

    def down(src, dst, i, x):
        return pltpu.make_async_remote_copy(
            src_ref=src.at[i], dst_ref=dst.at[i], send_sem=total_sem.at[1], recv_sem=downrecv_sem.at[slot["down", (x + 3) % 4](i)],
            device_id={"south": ring[0]}, device_id_type=pl.DeviceIdType.MESH,
        )

    def totals_sent(side, n):
        ref = total.at[pl.ds(0, n)]
        pltpu.make_async_remote_copy(
            src_ref=ref, dst_ref=ref, send_sem=total_sem.at[side], recv_sem=uprecv_sem.at[0],
            device_id={"south": ring[1 - side]}, device_id_type=pl.DeviceIdType.MESH,
        ).wait_send()

    first = {
        0: (("G", down, ahigh), ("A", up, below), ("B", up, below), ("H", up, below)),
        1: (("G", up, alow), ("H", down, ahigh)),
        2: (("H", up, alow), ("B", down, ahigh)),
        3: (),
    }

    def send_totals(c):
        for x, sends in first.items():
            ready = []
            latest = {"up": 0, "down": 0}
            for w, go, target in sends:
                key = "up" if go is up else "down"
                latest[key] = max(latest[key], max(WAYS[w]))
                if latest[key] == c:
                    ready.append((w, go, target))
            if ready:
                @pl.when(place["south"] == x)
                def _():
                    for w, go, target in ready:
                        for i in ways[w]:
                            go(total, target, i, x).start()

    first_row = lax.broadcasted_iota(jnp.int32, (8, nm), 0) == 0
    last_row = lax.broadcasted_iota(jnp.int32, (8, nm), 0) == 7

    for t in range(STEPS):
        src, dst = bufs[t % 2], bufs[(t + 1) % 2]
        last = t == STEPS - 1

        def chunk(c, _, t=t, src=src, dst=dst, last=last):
            buf = bufs[t % 2]
            arrived("south", xrecv_sem.at[t % 2, c], buf.at[0, pl.ds(1, ROWS)], buf.at[0, pl.ds(1, 2 * ROWS)])
            rows = pl.ds(c * ROWS, ROWS)
            arrived("down", zrecv_sem.at[t % 2, c], zrecv.at[t, 0, rows], zrecv.at[t, pl.ds(0, 2), rows])
            on(jnp.logical_and(has["east"][0], c == 0), lambda: y_copy(t, 1).wait_recv())
            on(jnp.logical_and(has["east"][1], c == chunks - 1), lambda: y_copy(t, 0).wait_recv())

            def row(r, _):
                i = c * ROWS + r
                acc = None
                for j in range(nj):
                    mid = src[1 + j, 1 + i]
                    above = pltpu.roll(mid, 1, 0)
                    under = pltpu.roll(mid, nk - 1, 0)
                    zl = zrecv[t, 0, i, j : j + 1]
                    zh = zrecv[t, 1, i, j : j + 1]
                    above = jnp.concatenate([jnp.where(first_row, zl, above[:8]), above[8:]], axis=0)
                    under = jnp.concatenate([under[:-8], jnp.where(last_row, zh, under[-8:])], axis=0)
                    spread = src[j, 1 + i] + src[2 + j, 1 + i] + src[1 + j, i] + src[1 + j, 2 + i] + above + under - 6.0 * mid
                    new = 2.0 * mid - dst[1 + j, 1 + i] + speed[j, i] * spread
                    dst[1 + j, 1 + i] = new
                    if last:
                        acc = new if acc is None else acc + new
                    else:
                        zsend[t + 1, 0, i, j : j + 1] = new[0:1]
                        zsend[t + 1, 1, i, j : j + 1] = new[nk - 1 : nk]
                if last:
                    total[i] = acc
                return 0

            lax.fori_loop(0, ROWS, row, 0)
            if not last:
                for side in (1, 0):
                    on(has["south"][side], lambda: x_copy(t + 1, side, c).start())
                z_start(t + 1, c)
                on(jnp.logical_and(has["east"][0], c == 0), lambda: y_copy(t + 1, 0).start())
                on(jnp.logical_and(has["east"][1], c == chunks - 1), lambda: y_copy(t + 1, 1).start())
            return 0

        if t >= 1:
            sent_faces(t - 1)
        if last:
            for c in range(chunks):
                chunk(c, 0)
                send_totals(c)
        else:
            lax.fori_loop(0, chunks, chunk, 0)

    def got_up(i, x):
        up(total, below, i, x - 1).wait_recv()

    def got_down(i, x):
        down(total, below, i, (x + 1) % 4).wait_recv()

    def pairs(a, b):
        for k in range(max(len(ways[a]), len(ways[b]))):
            yield ways[a][k] if k < len(ways[a]) else None, ways[b][k] if k < len(ways[b]) else None

    @pl.when(place["south"] == 0)
    def _():
        for w, target in (("H", ahigh), ("B", below)):
            for i in ways[w]:
                got_down(i, 0)
                shigh[i] = total[i] + ahigh[i]
                down(shigh, target, i, 0).start()
        for i in range(ni):
            below[i] = jnp.zeros((nk, nm), jnp.float32)
        totals_sent(0, sum(len(ways[w]) for w in "ABH"))
        totals_sent(1, sum(len(ways[w]) for w in "GHB"))

    @pl.when(place["south"] == 1)
    def _():
        def relay_up(i):
            got_up(i, 1)
            slow[i] = below[i] + total[i]
            up(slow, below, i, 1).start()

        for a, b in pairs("A", "B"):
            if a is not None:
                relay_up(a)
            if b is not None:
                got_down(b, 1)
                shigh[b] = total[b] + ahigh[b]
                down(shigh, ahigh, b, 1).start()
        for i in ways["B"]:
            relay_up(i)
        for i in ways["G"]:
            got_down(i, 1)
        for i in ways["H"]:
            got_up(i, 1)
        totals_sent(0, sum(len(ways[w]) for w in "GAB"))
        totals_sent(1, sum(len(ways[w]) for w in "HB"))

    @pl.when(place["south"] == 2)
    def _():
        for i in ways["G"]:
            got_up(i, 2)
            slow[i] = alow[i] + total[i]
            up(slow, alow, i, 2).start()
        for g, a in pairs("G", "A"):
            if g is not None:
                got_down(g, 2)
                down(ahigh, below, g, 2).start()
                below[g] = ahigh[g] + alow[g]
            if a is not None:
                got_up(a, 2)
                slow[a] = below[a] + total[a]
                up(slow, below, a, 2).start()
        for i in ways["B"]:
            got_up(i, 2)
        for i in ways["H"]:
            got_down(i, 2)
        totals_sent(0, sum(len(ways[w]) for w in "HGA"))
        totals_sent(1, sum(len(ways[w]) for w in "BG"))

    @pl.when(place["south"] == 3)
    def _():
        for i in ways["G"]:
            got_down(i, 3)
            down(ahigh, ahigh, i, 3).start()
        for i in ways["H"]:
            got_down(i, 3)
            down(ahigh, below, i, 3).start()
            got_up(i, 3)
            below[i] = ahigh[i] + alow[i]
        for i in ways["G"]:
            got_up(i, 3)
            below[i] = ahigh[i] + alow[i]
        for i in ways["A"]:
            got_up(i, 3)
        for i in ways["B"]:
            got_down(i, 3)
        totals_sent(1, sum(len(ways[w]) for w in "GH"))

    sent_faces(STEPS - 1)
    for side in (0, 1):
        ref = zsend.at[:, side]
        on(has["down"][side], lambda: remote(ref, ref, zsend_sem.at[side], zrecv_sem.at[0, 0], "down", side).wait_send())


def outputs_kernel(grid_j, field, below, running, end, stage, out_sem, field_sem):
    nj, ni, nk, nm = end.shape
    rows = 2
    groups = ni // rows
    whole = pltpu.make_async_copy(field.at[pl.ds(1, nj), pl.ds(1, ni)], end, field_sem)
    whole.start()

    def out(g):
        at = pl.ds(g * rows, rows)
        return pltpu.make_async_copy(stage.at[:, at], running.at[:, at], out_sem)

    def group(g, _):
        for r in range(rows):
            i = g * rows + r
            acc = below[i]
            for j in range(nj):
                acc = acc + field[1 + j, 1 + i]
                stage[j, i] = acc * (1.0 / grid_j)
        out(g).start()
        return 0

    lax.fori_loop(0, groups, group, 0)

    pltpu.make_async_copy(stage, running, out_sem).wait()
    whole.wait()


def shards(field_now, earlier, speed_square):
    shape = field_now.shape
    nj, ni, nk, nm = shape
    padded = (nj + 2, ni + 2, nk, nm)
    chunks = ni // ROWS
    grid_j = nj * lax.axis_size("south")
    dma = pltpu.SemaphoreType.DMA
    anyspace = pl.BlockSpec(memory_space=pltpu.HBM)
    vmem = pl.BlockSpec(memory_space=pltpu.VMEM)
    f32 = jnp.float32
    field, below = pl.pallas_call(
        functools.partial(steps_kernel, grid_j),
        out_shape=(pltpu.VMEM(padded, f32), pltpu.VMEM((ni, nk, nm), f32)),
        in_specs=[anyspace] * 3,
        out_specs=(vmem, vmem),
        scratch_shapes=[
            pltpu.VMEM(padded, f32),
            pltpu.VMEM(shape, f32),
            pltpu.VMEM((STEPS, 2, ni, nj, nm), f32),
            pltpu.VMEM((STEPS, 2, ni, nj, nm), f32),
            *[pltpu.VMEM((ni, nk, nm), f32)] * 5,
            pltpu.VMEM((2, ROWS, nk, nm), f32),
            dma((4,)),
            dma((2, 2)), dma((2, chunks)),
            dma((2, 2)), dma((2, 2)),
            dma((2,)), dma((2, chunks)),
            dma((2,)), dma((3 * ni // 4,)), dma((3 * ni // 4,)),
        ],
        compiler_params=pltpu.CompilerParams(
            collective_id=0, has_side_effects=True, vmem_limit_bytes=40 * 1024 * 1024,
        ),
        name="steps",
    )(field_now, earlier, speed_square)
    return pl.pallas_call(
        functools.partial(outputs_kernel, grid_j),
        out_shape=(jax.ShapeDtypeStruct(shape, f32), jax.ShapeDtypeStruct(shape, f32)),
        in_specs=[vmem, vmem],
        out_specs=(anyspace, anyspace),
        scratch_shapes=[pltpu.VMEM(shape, f32), dma, dma],
        compiler_params=pltpu.CompilerParams(vmem_limit_bytes=32 * 1024 * 1024),
        name="outputs",
    )(field, below)


def solution(mesh):
    placed = P(*AXES, None)
    return jax.shard_map(
        shards,
        mesh=mesh,
        in_specs=(placed, placed, placed),
        out_specs=(placed, placed),
        check_vma=False,
    )
```

```python
import functools

import jax
import jax.numpy as jnp
from jax import lax
from jax.experimental import pallas as pl
from jax.experimental.pallas import tpu as pltpu
from jax.sharding import PartitionSpec as P

STEPS = 4
ROWS = 4
AXES = ("south", "east", "down")
WAYS = {"G": (0,), "H": (1,), "A": (2,), "B": (3,)}


def steps_kernel(
    grid_j, u0, e0, s0, field, below, prev, speed, zsend, zrecv, total, alow, ahigh, slow, shigh, lead,
    load_sem, xsend_sem, xrecv_sem, ysend_sem, yrecv_sem, zsend_sem, zrecv_sem, total_sem, uprecv_sem, downrecv_sem,
):
    nj, ni, nk, nm = s0.shape
    chunks = ni // ROWS
    place = {a: lax.axis_index(a) for a in AXES}
    count = {a: lax.axis_size(a) for a in AXES}
    has = {a: (place[a] > 0, place[a] < count[a] - 1) for a in AXES}
    peer = {a: (place[a] - 1, place[a] + 1) for a in AXES}

    barrier = pltpu.get_barrier_semaphore()

    def greet(a):
        for side in (0, 1):
            @pl.when(has[a][side])
            def _():
                pl.semaphore_signal(barrier, inc=1, device_id={a: peer[a][side]}, device_id_type=pl.DeviceIdType.MESH)
        return has[a][0].astype(jnp.int32) + has[a][1].astype(jnp.int32)

    odd = lax.rem(place["east"], 2) == 1
    greeted = greet("south") + greet("down")
    beside = has["east"][0].astype(jnp.int32) + has["east"][1].astype(jnp.int32)

    inner = (pl.ds(1, nj), pl.ds(1, ni))
    leads = [
        pltpu.make_async_copy(u0.at[(nj - 1) * side, pl.ds(0, ROWS)], lead.at[side], load_sem.at[3]) for side in (0, 1)
    ]
    loads = [
        pltpu.make_async_copy(u0, field.at[inner], load_sem.at[0]),
        pltpu.make_async_copy(e0, prev.at[inner], load_sem.at[1]),
        pltpu.make_async_copy(s0, speed, load_sem.at[2]),
    ]
    for load in leads + loads:
        load.start()
    ring = (lax.rem(place["south"] + count["south"] - 1, count["south"]), lax.rem(place["south"] + 1, count["south"]))
    pltpu.make_async_copy(u0.at[pl.ds(0, 2), pl.ds(0, ROWS)], lead, load_sem.at[3]).wait()
    pl.semaphore_wait(barrier, greeted + jnp.where(odd, 0, beside))
    greet("east")

    bufs = (field, prev)

    def remote(src, dst, send_sem, recv_sem, axis, side):
        return pltpu.make_async_remote_copy(
            src_ref=src, dst_ref=dst, send_sem=send_sem, recv_sem=recv_sem,
            device_id={axis: peer[axis][side]}, device_id_type=pl.DeviceIdType.MESH,
        )

    def x_copy(t, side, c, src=None):
        buf = bufs[t % 2]
        rows = pl.ds(1 + c * ROWS, ROWS)
        own, dst = (nj if side else 1), (0 if side else nj + 1)
        src = buf.at[own, rows] if src is None else src
        return remote(src, buf.at[dst, rows], xsend_sem.at[t % 2, side], xrecv_sem.at[t % 2, c], "south", side)

    def y_copy(t, side, src=None):
        buf = bufs[t % 2]
        own, dst = (ni if side else 1), (0 if side else ni + 1)
        src = buf.at[pl.ds(1, nj), own] if src is None else src
        return remote(src, buf.at[pl.ds(1, nj), dst], ysend_sem.at[t % 2, side], yrecv_sem.at[t % 2, 1 - side], "east", side)

    def z_copy(t, side, c):
        rows = pl.ds(c * ROWS, ROWS)
        return remote(
            zsend.at[t, side, rows], zrecv.at[t, 1 - side, rows],
            zsend_sem.at[side], zrecv_sem.at[t % 2, c], "down", side,
        )

    def arrived(axis, sem, one, both):
        two = jnp.logical_and(*has[axis])
        for pred, ref in ((two, both), (jnp.logical_not(two), one)):
            @pl.when(pred)
            def _():
                remote(ref, ref, zsend_sem.at[0], sem, axis, 0).wait_recv()

    def sent(axis, sems, ref):
        for side in (0, 1):
            on(has[axis][side], lambda: remote(ref, ref, sems(side), zrecv_sem.at[0, 0], axis, side).wait_send())

    def sent_faces(t):
        sent("south", lambda side: xsend_sem.at[t % 2, side], field.at[0, pl.ds(1, ni)])
        sent("east", lambda side: ysend_sem.at[t % 2, side], field.at[pl.ds(1, nj), 0])

    def on(pred, action):
        @pl.when(pred)
        def _():
            action()

    for c in range(chunks):
        rows = pl.ds(c * ROWS, ROWS)
        for side in (1, 0):
            face = u0.at[nj - 1 if side else 0, rows] if c else lead.at[side]
            on(has["south"][side], lambda: x_copy(0, side, c, face).start())
    on(odd, lambda: pl.semaphore_wait(barrier, beside))
    for side in (1, 0):
        on(has["east"][side], lambda: y_copy(0, side, u0.at[:, ni - 1 if side else 0]).start())

    for buf in bufs:
        for side in (0, 1):
            @pl.when(jnp.logical_not(has["south"][side]))
            def _():
                def fill(i, _):
                    buf[(nj + 1) * side, i] = jnp.zeros((nk, nm), jnp.float32)
                    return 0
                lax.fori_loop(0, ni + 2, fill, 0)

            @pl.when(jnp.logical_not(has["east"][side]))
            def _():
                def fill(j, _):
                    buf[j, (ni + 1) * side] = jnp.zeros((nk, nm), jnp.float32)
                    return 0
                lax.fori_loop(1, nj + 1, fill, 0)
    for side in (0, 1):
        @pl.when(jnp.logical_not(has["down"][side]))
        def _():
            def fill(i, _):
                for t in range(STEPS):
                    zrecv[t, side, i] = jnp.zeros((nj, nm), jnp.float32)
                return 0
            lax.fori_loop(0, ni, fill, 0)

    loads[0].wait()

    def pack(i, _):
        for j in range(nj):
            zsend[0, 0, i, j : j + 1] = field[1 + j, 1 + i, 0:1]
            zsend[0, 1, i, j : j + 1] = field[1 + j, 1 + i, nk - 1 : nk]
        return 0

    lax.fori_loop(0, ni, pack, 0)

    def z_start(t, c):
        for side in (1, 0):
            on(has["down"][side], lambda: z_copy(t, side, c).start())

    def send_all_z(c, _):
        z_start(0, c)
        return 0

    lax.fori_loop(0, chunks, send_all_z, 0)
    loads[1].wait()
    loads[2].wait()

    ways = {w: [c * ROWS + r for c in cs for r in range(ROWS)] for w, cs in WAYS.items()}
    came = {"up": {1: "ABH", 2: "GAB", 3: "HGA"}, "down": {0: "HB", 1: "BG", 2: "GH", 3: "GHB"}}
    slot = {(key, x): [i for w in ws for i in ways[w]].index for key, at in came.items() for x, ws in at.items()}

    def up(src, dst, i, x):
        return pltpu.make_async_remote_copy(
            src_ref=src.at[i], dst_ref=dst.at[i], send_sem=total_sem.at[0], recv_sem=uprecv_sem.at[slot["up", x + 1](i)],
            device_id={"south": ring[1]}, device_id_type=pl.DeviceIdType.MESH,
        )

    def down(src, dst, i, x):
        return pltpu.make_async_remote_copy(
            src_ref=src.at[i], dst_ref=dst.at[i], send_sem=total_sem.at[1], recv_sem=downrecv_sem.at[slot["down", (x + 3) % 4](i)],
            device_id={"south": ring[0]}, device_id_type=pl.DeviceIdType.MESH,
        )

    def totals_sent(side, n):
        ref = total.at[pl.ds(0, n)]
        pltpu.make_async_remote_copy(
            src_ref=ref, dst_ref=ref, send_sem=total_sem.at[side], recv_sem=uprecv_sem.at[0],
            device_id={"south": ring[1 - side]}, device_id_type=pl.DeviceIdType.MESH,
        ).wait_send()

    first = {
        0: (("G", down, ahigh), ("A", up, below), ("B", up, below), ("H", up, below)),
        1: (("G", up, alow), ("H", down, ahigh)),
        2: (("H", up, alow), ("B", down, ahigh)),
        3: (),
    }

    def send_totals(c):
        for x, sends in first.items():
            ready = []
            latest = {"up": 0, "down": 0}
            for w, go, target in sends:
                key = "up" if go is up else "down"
                latest[key] = max(latest[key], max(WAYS[w]))
                if latest[key] == c:
                    ready.append((w, go, target))
            if ready:
                @pl.when(place["south"] == x)
                def _():
                    for w, go, target in ready:
                        for i in ways[w]:
                            go(total, target, i, x).start()

    first_row = lax.broadcasted_iota(jnp.int32, (8, nm), 0) == 0
    last_row = lax.broadcasted_iota(jnp.int32, (8, nm), 0) == 7

    for t in range(STEPS):
        src, dst = bufs[t % 2], bufs[(t + 1) % 2]
        last = t == STEPS - 1

        def chunk(c, _, t=t, src=src, dst=dst, last=last):
            buf = bufs[t % 2]
            arrived("south", xrecv_sem.at[t % 2, c], buf.at[0, pl.ds(1, ROWS)], buf.at[0, pl.ds(1, 2 * ROWS)])
            rows = pl.ds(c * ROWS, ROWS)
            arrived("down", zrecv_sem.at[t % 2, c], zrecv.at[t, 0, rows], zrecv.at[t, pl.ds(0, 2), rows])
            on(jnp.logical_and(has["east"][0], c == 0), lambda: y_copy(t, 1).wait_recv())
            on(jnp.logical_and(has["east"][1], c == chunks - 1), lambda: y_copy(t, 0).wait_recv())

            def row(r, _):
                i = c * ROWS + r
                acc = None
                for j in range(nj):
                    mid = src[1 + j, 1 + i]
                    above = pltpu.roll(mid, 1, 0)
                    under = pltpu.roll(mid, nk - 1, 0)
                    zl = zrecv[t, 0, i, j : j + 1]
                    zh = zrecv[t, 1, i, j : j + 1]
                    above = jnp.concatenate([jnp.where(first_row, zl, above[:8]), above[8:]], axis=0)
                    under = jnp.concatenate([under[:-8], jnp.where(last_row, zh, under[-8:])], axis=0)
                    spread = src[j, 1 + i] + src[2 + j, 1 + i] + src[1 + j, i] + src[1 + j, 2 + i] + above + under - 6.0 * mid
                    new = 2.0 * mid - dst[1 + j, 1 + i] + speed[j, i] * spread
                    dst[1 + j, 1 + i] = new
                    if last:
                        acc = new if acc is None else acc + new
                    else:
                        zsend[t + 1, 0, i, j : j + 1] = new[0:1]
                        zsend[t + 1, 1, i, j : j + 1] = new[nk - 1 : nk]
                if last:
                    total[i] = acc
                return 0

            lax.fori_loop(0, ROWS, row, 0)
            if not last:
                for side in (1, 0):
                    on(has["south"][side], lambda: x_copy(t + 1, side, c).start())
                z_start(t + 1, c)
                on(jnp.logical_and(has["east"][0], c == 0), lambda: y_copy(t + 1, 0).start())
                on(jnp.logical_and(has["east"][1], c == chunks - 1), lambda: y_copy(t + 1, 1).start())
            return 0

        if t >= 1:
            sent_faces(t - 1)
        if last:
            for c in range(chunks):
                chunk(c, 0)
                send_totals(c)
        else:
            lax.fori_loop(0, chunks, chunk, 0)

    def got_up(i, x):
        up(total, below, i, x - 1).wait_recv()

    def got_down(i, x):
        down(total, below, i, (x + 1) % 4).wait_recv()

    def pairs(a, b):
        for k in range(max(len(ways[a]), len(ways[b]))):
            yield ways[a][k] if k < len(ways[a]) else None, ways[b][k] if k < len(ways[b]) else None

    @pl.when(place["south"] == 0)
    def _():
        for w, target in (("H", ahigh), ("B", below)):
            for i in ways[w]:
                got_down(i, 0)
                shigh[i] = total[i] + ahigh[i]
                down(shigh, target, i, 0).start()
        for i in range(ni):
            below[i] = jnp.zeros((nk, nm), jnp.float32)
        totals_sent(0, sum(len(ways[w]) for w in "ABH"))
        totals_sent(1, sum(len(ways[w]) for w in "GHB"))

    @pl.when(place["south"] == 1)
    def _():
        def relay_up(i):
            got_up(i, 1)
            slow[i] = below[i] + total[i]
            up(slow, below, i, 1).start()

        for a, b in pairs("A", "B"):
            if a is not None:
                relay_up(a)
            if b is not None:
                got_down(b, 1)
                shigh[b] = total[b] + ahigh[b]
                down(shigh, ahigh, b, 1).start()
        for i in ways["B"]:
            relay_up(i)
        for i in ways["G"]:
            got_down(i, 1)
        for i in ways["H"]:
            got_up(i, 1)
        totals_sent(0, sum(len(ways[w]) for w in "GAB"))
        totals_sent(1, sum(len(ways[w]) for w in "HB"))

    @pl.when(place["south"] == 2)
    def _():
        for i in ways["G"]:
            got_up(i, 2)
            slow[i] = alow[i] + total[i]
            up(slow, alow, i, 2).start()
        for g, a in pairs("G", "A"):
            if g is not None:
                got_down(g, 2)
                down(ahigh, below, g, 2).start()
                below[g] = ahigh[g] + alow[g]
            if a is not None:
                got_up(a, 2)
                slow[a] = below[a] + total[a]
                up(slow, below, a, 2).start()
        for i in ways["B"]:
            got_up(i, 2)
        for i in ways["H"]:
            got_down(i, 2)
        totals_sent(0, sum(len(ways[w]) for w in "HGA"))
        totals_sent(1, sum(len(ways[w]) for w in "BG"))

    @pl.when(place["south"] == 3)
    def _():
        for i in ways["G"]:
            got_down(i, 3)
            down(ahigh, ahigh, i, 3).start()
        for i in ways["H"]:
            got_down(i, 3)
            down(ahigh, below, i, 3).start()
            got_up(i, 3)
            below[i] = ahigh[i] + alow[i]
        for i in ways["G"]:
            got_up(i, 3)
            below[i] = ahigh[i] + alow[i]
        for i in ways["A"]:
            got_up(i, 3)
        for i in ways["B"]:
            got_down(i, 3)
        totals_sent(1, sum(len(ways[w]) for w in "GH"))

    sent_faces(STEPS - 1)
    for side in (0, 1):
        ref = zsend.at[:, side]
        on(has["down"][side], lambda: remote(ref, ref, zsend_sem.at[side], zrecv_sem.at[0, 0], "down", side).wait_send())


def outputs_kernel(grid_j, field, below, running, end, stage, out_sem, field_sem):
    nj, ni, nk, nm = end.shape
    rows = 2
    groups = ni // rows
    whole = pltpu.make_async_copy(field.at[pl.ds(1, nj), pl.ds(1, ni)], end, field_sem)
    whole.start()

    def out(g):
        at = pl.ds(g * rows, rows)
        return pltpu.make_async_copy(stage.at[:, at], running.at[:, at], out_sem)

    def group(g, _):
        for r in range(rows):
            i = g * rows + r
            acc = below[i]
            for j in range(nj):
                acc = acc + field[1 + j, 1 + i]
                stage[j, i] = acc * (1.0 / grid_j)
        out(g).start()
        return 0

    lax.fori_loop(0, groups, group, 0)

    pltpu.make_async_copy(stage, running, out_sem).wait()
    whole.wait()


def shards(field_now, earlier, speed_square):
    shape = field_now.shape
    nj, ni, nk, nm = shape
    padded = (nj + 2, ni + 2, nk, nm)
    chunks = ni // ROWS
    grid_j = nj * lax.axis_size("south")
    dma = pltpu.SemaphoreType.DMA
    anyspace = pl.BlockSpec(memory_space=pltpu.HBM)
    vmem = pl.BlockSpec(memory_space=pltpu.VMEM)
    f32 = jnp.float32
    field, below = pl.pallas_call(
        functools.partial(steps_kernel, grid_j),
        out_shape=(pltpu.VMEM(padded, f32), pltpu.VMEM((ni, nk, nm), f32)),
        in_specs=[anyspace] * 3,
        out_specs=(vmem, vmem),
        scratch_shapes=[
            pltpu.VMEM(padded, f32),
            pltpu.VMEM(shape, f32),
            pltpu.VMEM((STEPS, 2, ni, nj, nm), f32),
            pltpu.VMEM((STEPS, 2, ni, nj, nm), f32),
            *[pltpu.VMEM((ni, nk, nm), f32)] * 5,
            pltpu.VMEM((2, ROWS, nk, nm), f32),
            dma((4,)),
            dma((2, 2)), dma((2, chunks)),
            dma((2, 2)), dma((2, 2)),
            dma((2,)), dma((2, chunks)),
            dma((2,)), dma((3 * ni // 4,)), dma((3 * ni // 4,)),
        ],
        compiler_params=pltpu.CompilerParams(
            collective_id=0, has_side_effects=True, vmem_limit_bytes=40 * 1024 * 1024,
        ),
        name="steps",
    )(field_now, earlier, speed_square)
    return pl.pallas_call(
        functools.partial(outputs_kernel, grid_j),
        out_shape=(jax.ShapeDtypeStruct(shape, f32), jax.ShapeDtypeStruct(shape, f32)),
        in_specs=[vmem, vmem],
        out_specs=(anyspace, anyspace),
        scratch_shapes=[pltpu.VMEM(shape, f32), dma, dma],
        compiler_params=pltpu.CompilerParams(vmem_limit_bytes=32 * 1024 * 1024),
        name="outputs",
    )(field, below)


def solution(mesh):
    placed = P(*AXES, None)
    return jax.shard_map(
        shards,
        mesh=mesh,
        in_specs=(placed, placed, placed),
        out_specs=(placed, placed),
        check_vma=False,
    )
```

```python
import functools

import jax
import jax.numpy as jnp
from jax import lax
from jax.experimental import pallas as pl
from jax.experimental.pallas import tpu as pltpu
from jax.sharding import PartitionSpec as P

STEPS = 4
ROWS = 4
AXES = ("south", "east", "down")

TABLES = (
    (
        "GHBHAGAGHBGABBHA",
        {(0, "up"): (8, 6, 11, 4, 12, 15, 13, 2, 9, 3, 14, 1), (0, "down"): (7, 0, 5, 10), (1, "up"): (5, 7, 10, 0), (1, "down"): (8, 1, 3, 14), (2, "up"): (3, 8, 1, 14), (2, "down"): (2, 9, 12, 13)},
        {0: ((-1, 8), (-1, 1), (-1, 3), (-1, 14), (-1, 2), (-1, 9), (-1, 12), (-1, 13)), 1: ((-1, 2), (1, 6), (-1, 9), (1, 11), (-1, 12), (1, 4), (-1, 13), (1, 12), (1, 15), (1, 13), (1, 2), (1, 9)), 2: ((1, 5), (1, 7), (1, 10), (-1, 7), (1, 0), (-1, 0), (1, 6), (-1, 5), (1, 11), (-1, 10), (1, 4), (1, 15)), 3: ((-1, 7), (-1, 0), (-1, 5), (-1, 10), (-1, 8), (-1, 1), (-1, 3), (-1, 14))},
    ),
    (
        "HGGBBGGBHGHBHAAB",
        {(0, "up"): (4, 8, 10, 14, 7, 13, 15, 3, 11, 12, 0), (0, "down"): (2, 9, 1, 6, 5), (1, "up"): (6, 5, 2, 1, 9), (1, "down"): (0, 10, 8, 12), (2, "up"): (0, 8, 10, 12), (2, "down"): (11, 7, 3, 15, 4)},
        {0: ((-1, 0), (-1, 10), (-1, 8), (-1, 12), (-1, 11), (-1, 7), (-1, 3), (-1, 15), (-1, 4)), 1: ((1, 4), (-1, 11), (-1, 7), (-1, 3), (1, 14), (-1, 15), (1, 7), (-1, 4), (1, 13), (1, 15), (1, 3), (1, 11)), 2: ((1, 6), (1, 5), (1, 2), (-1, 2), (1, 1), (-1, 9), (1, 9), (-1, 1), (-1, 6), (1, 14), (-1, 5), (1, 13)), 3: ((-1, 2), (-1, 9), (-1, 1), (-1, 6), (-1, 5), (-1, 0), (-1, 10), (-1, 8), (-1, 12))},
    ),
)
ENDS = {0: [], 1: [("down", "G"), ("up", "H")], 2: [("down", "H"), ("up", "B")], 3: [("up", "H"), ("up", "G"), ("down", "B"), ("up", "A")]}
PLAIN = {(1, "up"): "ABH", (2, "up"): "AB", (3, "up"): "A", (1, "down"): "G", (2, "down"): "H", (3, "down"): "B", (0, "down"): ""}


def steps_kernel(
    grid_j, u0, e0, s0, field, below, prev, speed, zsend, zrecv, total, alow, ahigh, slow, shigh, lead,
    load_sem, xsend_sem, xrecv_sem, ysend_sem, yrecv_sem, zsend_sem, zrecv_sem, total_sem, uprecv_sem, downrecv_sem,
):
    nj, ni, nk, nm = s0.shape
    chunks = ni // ROWS
    place = {a: lax.axis_index(a) for a in AXES}
    count = {a: lax.axis_size(a) for a in AXES}
    has = {a: (place[a] > 0, place[a] < count[a] - 1) for a in AXES}
    peer = {a: (place[a] - 1, place[a] + 1) for a in AXES}

    barrier = pltpu.get_barrier_semaphore()

    def greet(a):
        for side in (0, 1):
            @pl.when(has[a][side])
            def _():
                pl.semaphore_signal(barrier, inc=1, device_id={a: peer[a][side]}, device_id_type=pl.DeviceIdType.MESH)
        return has[a][0].astype(jnp.int32) + has[a][1].astype(jnp.int32)

    odd = lax.rem(place["east"], 2) == 1
    greeted = greet("south") + greet("down")
    beside = has["east"][0].astype(jnp.int32) + has["east"][1].astype(jnp.int32)

    inner = (pl.ds(1, nj), pl.ds(1, ni))
    leads = [
        pltpu.make_async_copy(u0.at[(nj - 1) * side, pl.ds(0, ROWS)], lead.at[side], load_sem.at[3]) for side in (0, 1)
    ]
    loads = [
        pltpu.make_async_copy(u0, field.at[inner], load_sem.at[0]),
        pltpu.make_async_copy(e0, prev.at[inner], load_sem.at[1]),
        pltpu.make_async_copy(s0, speed, load_sem.at[2]),
    ]
    for load in leads + loads:
        load.start()
    ring = (lax.rem(place["south"] + count["south"] - 1, count["south"]), lax.rem(place["south"] + 1, count["south"]))
    pltpu.make_async_copy(u0.at[pl.ds(0, 2), pl.ds(0, ROWS)], lead, load_sem.at[3]).wait()
    pl.semaphore_wait(barrier, greeted + jnp.where(odd, 0, beside))
    greet("east")

    bufs = (field, prev)

    def remote(src, dst, send_sem, recv_sem, axis, side):
        return pltpu.make_async_remote_copy(
            src_ref=src, dst_ref=dst, send_sem=send_sem, recv_sem=recv_sem,
            device_id={axis: peer[axis][side]}, device_id_type=pl.DeviceIdType.MESH,
        )

    def x_copy(t, side, c, src=None):
        buf = bufs[t % 2]
        rows = pl.ds(1 + c * ROWS, ROWS)
        own, dst = (nj if side else 1), (0 if side else nj + 1)
        src = buf.at[own, rows] if src is None else src
        return remote(src, buf.at[dst, rows], xsend_sem.at[t % 2, side], xrecv_sem.at[t % 2, c], "south", side)

    def y_copy(t, side, src=None):
        buf = bufs[t % 2]
        own, dst = (ni if side else 1), (0 if side else ni + 1)
        src = buf.at[pl.ds(1, nj), own] if src is None else src
        return remote(src, buf.at[pl.ds(1, nj), dst], ysend_sem.at[t % 2, side], yrecv_sem.at[t % 2, 1 - side], "east", side)

    def z_copy(t, side, c):
        rows = pl.ds(c * ROWS, ROWS)
        return remote(
            zsend.at[t, side, rows], zrecv.at[t, 1 - side, rows],
            zsend_sem.at[side], zrecv_sem.at[t % 2, c], "down", side,
        )

    def arrived(axis, sem, one, both):
        two = jnp.logical_and(*has[axis])
        for pred, ref in ((two, both), (jnp.logical_not(two), one)):
            @pl.when(pred)
            def _():
                remote(ref, ref, zsend_sem.at[0], sem, axis, 0).wait_recv()

    def sent(axis, sems, ref):
        for side in (0, 1):
            on(has[axis][side], lambda: remote(ref, ref, sems(side), zrecv_sem.at[0, 0], axis, side).wait_send())

    def sent_faces(t):
        sent("south", lambda side: xsend_sem.at[t % 2, side], field.at[0, pl.ds(1, ni)])
        sent("east", lambda side: ysend_sem.at[t % 2, side], field.at[pl.ds(1, nj), 0])

    def on(pred, action):
        @pl.when(pred)
        def _():
            action()

    for c in range(chunks):
        rows = pl.ds(c * ROWS, ROWS)
        for side in (1, 0):
            face = u0.at[nj - 1 if side else 0, rows] if c else lead.at[side]
            on(has["south"][side], lambda: x_copy(0, side, c, face).start())
    on(odd, lambda: pl.semaphore_wait(barrier, beside))
    for side in (1, 0):
        on(has["east"][side], lambda: y_copy(0, side, u0.at[:, ni - 1 if side else 0]).start())

    for buf in bufs:
        for side in (0, 1):
            @pl.when(jnp.logical_not(has["south"][side]))
            def _():
                def fill(i, _):
                    buf[(nj + 1) * side, i] = jnp.zeros((nk, nm), jnp.float32)
                    return 0
                lax.fori_loop(0, ni + 2, fill, 0)

            @pl.when(jnp.logical_not(has["east"][side]))
            def _():
                def fill(j, _):
                    buf[j, (ni + 1) * side] = jnp.zeros((nk, nm), jnp.float32)
                    return 0
                lax.fori_loop(1, nj + 1, fill, 0)
    for side in (0, 1):
        @pl.when(jnp.logical_not(has["down"][side]))
        def _():
            def fill(i, _):
                for t in range(STEPS):
                    zrecv[t, side, i] = jnp.zeros((nj, nm), jnp.float32)
                return 0
            lax.fori_loop(0, ni, fill, 0)

    loads[0].wait()

    def pack(i, _):
        for j in range(nj):
            zsend[0, 0, i, j : j + 1] = field[1 + j, 1 + i, 0:1]
            zsend[0, 1, i, j : j + 1] = field[1 + j, 1 + i, nk - 1 : nk]
        return 0

    lax.fori_loop(0, ni, pack, 0)

    def z_start(t, c):
        for side in (1, 0):
            on(has["down"][side], lambda: z_copy(t, side, c).start())

    def send_all_z(c, _):
        z_start(0, c)
        return 0

    lax.fori_loop(0, chunks, send_all_z, 0)
    loads[1].wait()
    loads[2].wait()

    recv = {"up": uprecv_sem, "down": downrecv_sem}

    def landing(x, way, w):
        return below if w in PLAIN[x, way] else (alow if way == "up" else ahigh)

    relays = [
        {x: [("up" if e > 0 else "down", i) for e, i in line] for x, line in table[2].items()} for table in TABLES
    ]
    slots = [{}, {}]
    for p in (0, 1):
        for x in range(4):
            for way in ("up", "down"):
                here = [i for k, i in relays[p][x] if k == way] + [w for k, w in ENDS[x] if k == way]
                slots[p].update({(x, way, key): n for n, key in enumerate(here)})

    def ring_copy(way, src, dst, recv_sem):
        return pltpu.make_async_remote_copy(
            src_ref=src, dst_ref=dst, send_sem=total_sem.at[int(way == "down")], recv_sem=recv_sem,
            device_id={"south": ring[int(way == "up")]}, device_id_type=pl.DeviceIdType.MESH,
        )

    def pass_on(p, x, way, i, src):
        to = (x + (1 if way == "up" else 3)) % 4
        w = TABLES[p][0][i]
        slot = slots[p][to, way, i] if (to, way, i) in slots[p] else slots[p][to, way, w]
        ring_copy(way, src.at[i], landing(to, way, w).at[i], recv[way].at[slot]).start()

    def here(p, x):
        return jnp.logical_and(odd == bool(p), place["south"] == x)

    def send_totals(c):
        for p in (0, 1):
            for x in range(3):
                ready = []
                for way in ("up", "down"):
                    latest = 0
                    for i in TABLES[p][1][x, way]:
                        latest = max(latest, i // ROWS)
                        if latest == c:
                            ready.append((way, i))
                if ready:
                    @pl.when(here(p, x))
                    def _():
                        for way, i in ready:
                            pass_on(p, x, way, i, total)

    first_row = lax.broadcasted_iota(jnp.int32, (8, nm), 0) == 0
    last_row = lax.broadcasted_iota(jnp.int32, (8, nm), 0) == 7

    for t in range(STEPS):
        src, dst = bufs[t % 2], bufs[(t + 1) % 2]
        last = t == STEPS - 1

        def chunk(c, _, t=t, src=src, dst=dst, last=last):
            buf = bufs[t % 2]
            arrived("south", xrecv_sem.at[t % 2, c], buf.at[0, pl.ds(1, ROWS)], buf.at[0, pl.ds(1, 2 * ROWS)])
            rows = pl.ds(c * ROWS, ROWS)
            arrived("down", zrecv_sem.at[t % 2, c], zrecv.at[t, 0, rows], zrecv.at[t, pl.ds(0, 2), rows])
            on(jnp.logical_and(has["east"][0], c == 0), lambda: y_copy(t, 1).wait_recv())
            on(jnp.logical_and(has["east"][1], c == chunks - 1), lambda: y_copy(t, 0).wait_recv())

            def row(r, _):
                i = c * ROWS + r
                acc = None
                for j in range(nj):
                    mid = src[1 + j, 1 + i]
                    above = pltpu.roll(mid, 1, 0)
                    under = pltpu.roll(mid, nk - 1, 0)
                    zl = zrecv[t, 0, i, j : j + 1]
                    zh = zrecv[t, 1, i, j : j + 1]
                    above = jnp.concatenate([jnp.where(first_row, zl, above[:8]), above[8:]], axis=0)
                    under = jnp.concatenate([under[:-8], jnp.where(last_row, zh, under[-8:])], axis=0)
                    spread = src[j, 1 + i] + src[2 + j, 1 + i] + src[1 + j, i] + src[1 + j, 2 + i] + above + under - 6.0 * mid
                    new = 2.0 * mid - dst[1 + j, 1 + i] + speed[j, i] * spread
                    dst[1 + j, 1 + i] = new
                    if last:
                        acc = new if acc is None else acc + new
                    else:
                        zsend[t + 1, 0, i, j : j + 1] = new[0:1]
                        zsend[t + 1, 1, i, j : j + 1] = new[nk - 1 : nk]
                if last:
                    total[i] = acc
                return 0

            lax.fori_loop(0, ROWS, row, 0)
            if not last:
                for side in (1, 0):
                    on(has["south"][side], lambda: x_copy(t + 1, side, c).start())
                z_start(t + 1, c)
                on(jnp.logical_and(has["east"][0], c == 0), lambda: y_copy(t + 1, 0).start())
                on(jnp.logical_and(has["east"][1], c == chunks - 1), lambda: y_copy(t + 1, 1).start())
            return 0

        if t >= 1:
            sent_faces(t - 1)
        if last:
            for c in range(chunks):
                chunk(c, 0)
                send_totals(c)
        else:
            lax.fori_loop(0, chunks, chunk, 0)

    for p, x in [(p, x) for p in (0, 1) for x in range(4)]:
        @pl.when(here(p, x))
        def _():
            ways, own, _ = TABLES[p]
            for way, i in relays[p][x]:
                came = landing(x, way, ways[i])
                ring_copy(way, came.at[i], came.at[i], recv[way].at[slots[p][x, way, i]]).wait_recv()
                if x == 3 or (x, way) == (2, "down"):
                    pass_on(p, x, way, i, came)
                else:
                    out = slow if way == "up" else shigh
                    out[i] = came[i] + total[i]
                    pass_on(p, x, way, i, out)
            if x == 2:
                for i in range(ni):
                    if ways[i] == "G":
                        below[i] = ahigh[i] + alow[i]
            for way, w in ENDS[x]:
                rows = [i for i in range(ni) if ways[i] == w]
                ref = total.at[pl.ds(0, len(rows))]
                ring_copy(way, ref, ref, recv[way].at[slots[p][x, way, w]]).wait_recv()
                if landing(x, way, w) is not below:
                    for i in rows:
                        below[i] = ahigh[i] + alow[i]
            if x == 0:
                for i in range(ni):
                    below[i] = jnp.zeros((nk, nm), jnp.float32)
            for way in ("up", "down"):
                count = len(own.get((x, way), ())) + sum(k == way for k, _ in relays[p][x])
                if count:
                    ref = total.at[pl.ds(0, count)]
                    ring_copy(way, ref, ref, uprecv_sem.at[0]).wait_send()

    sent_faces(STEPS - 1)
    for side in (0, 1):
        ref = zsend.at[:, side]
        on(has["down"][side], lambda: remote(ref, ref, zsend_sem.at[side], zrecv_sem.at[0, 0], "down", side).wait_send())


def outputs_kernel(grid_j, field, below, running, end, stage, out_sem, field_sem):
    nj, ni, nk, nm = end.shape
    rows = 2
    groups = ni // rows
    whole = pltpu.make_async_copy(field.at[pl.ds(1, nj), pl.ds(1, ni)], end, field_sem)
    whole.start()

    def out(g):
        at = pl.ds(g * rows, rows)
        return pltpu.make_async_copy(stage.at[:, at], running.at[:, at], out_sem)

    def group(g, _):
        for r in range(rows):
            i = g * rows + r
            acc = below[i]
            for j in range(nj):
                acc = acc + field[1 + j, 1 + i]
                stage[j, i] = acc * (1.0 / grid_j)
        out(g).start()
        return 0

    lax.fori_loop(0, groups, group, 0)

    pltpu.make_async_copy(stage, running, out_sem).wait()
    whole.wait()


def shards(field_now, earlier, speed_square):
    shape = field_now.shape
    nj, ni, nk, nm = shape
    padded = (nj + 2, ni + 2, nk, nm)
    chunks = ni // ROWS
    grid_j = nj * lax.axis_size("south")
    dma = pltpu.SemaphoreType.DMA
    anyspace = pl.BlockSpec(memory_space=pltpu.HBM)
    vmem = pl.BlockSpec(memory_space=pltpu.VMEM)
    f32 = jnp.float32
    field, below = pl.pallas_call(
        functools.partial(steps_kernel, grid_j),
        out_shape=(pltpu.VMEM(padded, f32), pltpu.VMEM((ni, nk, nm), f32)),
        in_specs=[anyspace] * 3,
        out_specs=(vmem, vmem),
        scratch_shapes=[
            pltpu.VMEM(padded, f32),
            pltpu.VMEM(shape, f32),
            pltpu.VMEM((STEPS, 2, ni, nj, nm), f32),
            pltpu.VMEM((STEPS, 2, ni, nj, nm), f32),
            *[pltpu.VMEM((ni, nk, nm), f32)] * 5,
            pltpu.VMEM((2, ROWS, nk, nm), f32),
            dma((4,)),
            dma((2, 2)), dma((2, chunks)),
            dma((2, 2)), dma((2, 2)),
            dma((2,)), dma((2, chunks)),
            dma((2,)), dma((9,)), dma((11,)),
        ],
        compiler_params=pltpu.CompilerParams(
            collective_id=0, has_side_effects=True, vmem_limit_bytes=40 * 1024 * 1024,
        ),
        name="steps",
    )(field_now, earlier, speed_square)
    return pl.pallas_call(
        functools.partial(outputs_kernel, grid_j),
        out_shape=(jax.ShapeDtypeStruct(shape, f32), jax.ShapeDtypeStruct(shape, f32)),
        in_specs=[vmem, vmem],
        out_specs=(anyspace, anyspace),
        scratch_shapes=[pltpu.VMEM(shape, f32), dma, dma],
        compiler_params=pltpu.CompilerParams(vmem_limit_bytes=32 * 1024 * 1024),
        name="outputs",
    )(field, below)


def solution(mesh):
    placed = P(*AXES, None)
    return jax.shard_map(
        shards,
        mesh=mesh,
        in_specs=(placed, placed, placed),
        out_specs=(placed, placed),
        check_vma=False,
    )
```

```python
import functools

import jax
import jax.numpy as jnp
from jax import lax
from jax.experimental import pallas as pl
from jax.experimental.pallas import tpu as pltpu
from jax.sharding import PartitionSpec as P

STEPS = 4
ROWS = 4
AXES = ("south", "east", "down")

TABLES = (
    (
        "HBBGGGHGHAAGABBH",
        {(0, "up"): (0, 8, 9, 10, 13, 12, 1, 2, 14, 6, 15), (0, "down"): (7, 4, 5, 3, 11), (1, "up"): (3, 5, 4, 11, 7), (1, "down"): (8, 6, 0, 15), (2, "up"): (6, 0, 8, 15), (2, "down"): (2, 13, 1, 14)},
        {0: ((-1, 8), (-1, 6), (-1, 0), (-1, 15), (-1, 2), (-1, 13), (-1, 1), (-1, 14)), 1: ((-1, 2), (1, 9), (-1, 13), (1, 10), (-1, 1), (1, 13), (-1, 14), (1, 12), (1, 1), (1, 2), (1, 14)), 2: ((1, 3), (1, 5), (1, 4), (-1, 7), (1, 11), (-1, 4), (1, 7), (-1, 5), (1, 9), (-1, 3), (1, 10), (-1, 11), (1, 12)), 3: ((-1, 7), (-1, 4), (-1, 5), (-1, 3), (-1, 11), (-1, 8), (-1, 6), (-1, 0), (-1, 15))},
    ),
    (
        "HGGBBGGGHBHBHAAB",
        {(0, "up"): (4, 8, 9, 12, 14, 13, 15, 3, 11, 10, 0), (0, "down"): (2, 7, 1, 6, 5), (1, "up"): (6, 5, 2, 1, 7), (1, "down"): (0, 10, 8, 12), (2, "up"): (0, 8, 10, 12), (2, "down"): (11, 9, 3, 15, 4)},
        {0: ((-1, 0), (-1, 10), (-1, 8), (-1, 12), (-1, 11), (-1, 9), (-1, 3), (-1, 15), (-1, 4)), 1: ((1, 4), (-1, 11), (-1, 9), (1, 9), (-1, 3), (-1, 15), (1, 14), (-1, 4), (1, 13), (1, 15), (1, 3), (1, 11)), 2: ((1, 6), (1, 5), (1, 2), (-1, 2), (1, 1), (-1, 7), (1, 7), (-1, 1), (-1, 6), (-1, 5), (1, 14), (1, 13)), 3: ((-1, 2), (-1, 7), (-1, 1), (-1, 6), (-1, 5), (-1, 0), (-1, 10), (-1, 8), (-1, 12))},
    ),
)
ENDS = {0: [], 1: [("down", "G"), ("up", "H")], 2: [("down", "H"), ("up", "B")], 3: [("up", "H"), ("up", "G"), ("down", "B"), ("up", "A")]}
PLAIN = {(1, "up"): "ABH", (2, "up"): "AB", (3, "up"): "A", (1, "down"): "G", (2, "down"): "H", (3, "down"): "B", (0, "down"): ""}


def steps_kernel(
    grid_j, u0, e0, s0, field, below, prev, speed, zsend, zrecv, total, alow, ahigh, slow, shigh, lead,
    load_sem, xsend_sem, xrecv_sem, ysend_sem, yrecv_sem, zsend_sem, zrecv_sem, total_sem, uprecv_sem, downrecv_sem,
):
    nj, ni, nk, nm = s0.shape
    chunks = ni // ROWS
    place = {a: lax.axis_index(a) for a in AXES}
    count = {a: lax.axis_size(a) for a in AXES}
    has = {a: (place[a] > 0, place[a] < count[a] - 1) for a in AXES}
    peer = {a: (place[a] - 1, place[a] + 1) for a in AXES}

    barrier = pltpu.get_barrier_semaphore()

    def greet(a):
        for side in (0, 1):
            @pl.when(has[a][side])
            def _():
                pl.semaphore_signal(barrier, inc=1, device_id={a: peer[a][side]}, device_id_type=pl.DeviceIdType.MESH)
        return has[a][0].astype(jnp.int32) + has[a][1].astype(jnp.int32)

    odd = lax.rem(place["east"], 2) == 1
    greeted = greet("south") + greet("down")
    beside = has["east"][0].astype(jnp.int32) + has["east"][1].astype(jnp.int32)

    inner = (pl.ds(1, nj), pl.ds(1, ni))
    leads = [
        pltpu.make_async_copy(u0.at[(nj - 1) * side, pl.ds(0, ROWS)], lead.at[side], load_sem.at[3]) for side in (0, 1)
    ]
    loads = [
        pltpu.make_async_copy(u0, field.at[inner], load_sem.at[0]),
        pltpu.make_async_copy(e0, prev.at[inner], load_sem.at[1]),
        pltpu.make_async_copy(s0, speed, load_sem.at[2]),
    ]
    for load in leads + loads:
        load.start()
    ring = (lax.rem(place["south"] + count["south"] - 1, count["south"]), lax.rem(place["south"] + 1, count["south"]))
    pltpu.make_async_copy(u0.at[pl.ds(0, 2), pl.ds(0, ROWS)], lead, load_sem.at[3]).wait()
    pl.semaphore_wait(barrier, greeted + jnp.where(odd, 0, beside))
    greet("east")

    bufs = (field, prev)

    def remote(src, dst, send_sem, recv_sem, axis, side):
        return pltpu.make_async_remote_copy(
            src_ref=src, dst_ref=dst, send_sem=send_sem, recv_sem=recv_sem,
            device_id={axis: peer[axis][side]}, device_id_type=pl.DeviceIdType.MESH,
        )

    def x_copy(t, side, c, src=None):
        buf = bufs[t % 2]
        rows = pl.ds(1 + c * ROWS, ROWS)
        own, dst = (nj if side else 1), (0 if side else nj + 1)
        src = buf.at[own, rows] if src is None else src
        return remote(src, buf.at[dst, rows], xsend_sem.at[t % 2, side], xrecv_sem.at[t % 2, c], "south", side)

    def y_copy(t, side, src=None):
        buf = bufs[t % 2]
        own, dst = (ni if side else 1), (0 if side else ni + 1)
        src = buf.at[pl.ds(1, nj), own] if src is None else src
        return remote(src, buf.at[pl.ds(1, nj), dst], ysend_sem.at[t % 2, side], yrecv_sem.at[t % 2, 1 - side], "east", side)

    def z_copy(t, side, c):
        rows = pl.ds(c * ROWS, ROWS)
        return remote(
            zsend.at[t, side, rows], zrecv.at[t, 1 - side, rows],
            zsend_sem.at[side], zrecv_sem.at[t % 2, c], "down", side,
        )

    def arrived(axis, sem, one, both):
        two = jnp.logical_and(*has[axis])
        for pred, ref in ((two, both), (jnp.logical_not(two), one)):
            @pl.when(pred)
            def _():
                remote(ref, ref, zsend_sem.at[0], sem, axis, 0).wait_recv()

    def sent(axis, sems, ref):
        for side in (0, 1):
            on(has[axis][side], lambda: remote(ref, ref, sems(side), zrecv_sem.at[0, 0], axis, side).wait_send())

    def sent_faces(t):
        sent("south", lambda side: xsend_sem.at[t % 2, side], field.at[0, pl.ds(1, ni)])
        sent("east", lambda side: ysend_sem.at[t % 2, side], field.at[pl.ds(1, nj), 0])

    def on(pred, action):
        @pl.when(pred)
        def _():
            action()

    for c in range(chunks):
        rows = pl.ds(c * ROWS, ROWS)
        for side in (1, 0):
            face = u0.at[nj - 1 if side else 0, rows] if c else lead.at[side]
            on(has["south"][side], lambda: x_copy(0, side, c, face).start())
    on(odd, lambda: pl.semaphore_wait(barrier, beside))
    for side in (1, 0):
        on(has["east"][side], lambda: y_copy(0, side, u0.at[:, ni - 1 if side else 0]).start())

    for buf in bufs:
        for side in (0, 1):
            @pl.when(jnp.logical_not(has["south"][side]))
            def _():
                def fill(i, _):
                    buf[(nj + 1) * side, i] = jnp.zeros((nk, nm), jnp.float32)
                    return 0
                lax.fori_loop(0, ni + 2, fill, 0)

            @pl.when(jnp.logical_not(has["east"][side]))
            def _():
                def fill(j, _):
                    buf[j, (ni + 1) * side] = jnp.zeros((nk, nm), jnp.float32)
                    return 0
                lax.fori_loop(1, nj + 1, fill, 0)
    for side in (0, 1):
        @pl.when(jnp.logical_not(has["down"][side]))
        def _():
            def fill(i, _):
                for t in range(STEPS):
                    zrecv[t, side, i] = jnp.zeros((nj, nm), jnp.float32)
                return 0
            lax.fori_loop(0, ni, fill, 0)

    loads[0].wait()

    def pack(i, _):
        for j in range(nj):
            zsend[0, 0, i, j : j + 1] = field[1 + j, 1 + i, 0:1]
            zsend[0, 1, i, j : j + 1] = field[1 + j, 1 + i, nk - 1 : nk]
        return 0

    lax.fori_loop(0, ni, pack, 0)

    def z_start(t, c):
        for side in (1, 0):
            on(has["down"][side], lambda: z_copy(t, side, c).start())

    def send_all_z(c, _):
        z_start(0, c)
        return 0

    lax.fori_loop(0, chunks, send_all_z, 0)
    loads[1].wait()
    loads[2].wait()

    recv = {"up": uprecv_sem, "down": downrecv_sem}

    def landing(x, way, w):
        return below if w in PLAIN[x, way] else (alow if way == "up" else ahigh)

    relays = [
        {x: [("up" if e > 0 else "down", i) for e, i in line] for x, line in table[2].items()} for table in TABLES
    ]
    slots = [{}, {}]
    for p in (0, 1):
        for x in range(4):
            for way in ("up", "down"):
                here = [i for k, i in relays[p][x] if k == way] + [w for k, w in ENDS[x] if k == way]
                slots[p].update({(x, way, key): n for n, key in enumerate(here)})

    def ring_copy(way, src, dst, recv_sem):
        return pltpu.make_async_remote_copy(
            src_ref=src, dst_ref=dst, send_sem=total_sem.at[int(way == "down")], recv_sem=recv_sem,
            device_id={"south": ring[int(way == "up")]}, device_id_type=pl.DeviceIdType.MESH,
        )

    def pass_on(p, x, way, i, src):
        to = (x + (1 if way == "up" else 3)) % 4
        w = TABLES[p][0][i]
        slot = slots[p][to, way, i] if (to, way, i) in slots[p] else slots[p][to, way, w]
        ring_copy(way, src.at[i], landing(to, way, w).at[i], recv[way].at[slot]).start()

    def here(p, x):
        return jnp.logical_and(odd == bool(p), place["south"] == x)

    def send_totals(c):
        for p in (0, 1):
            for x in range(3):
                ready = []
                for way in ("up", "down"):
                    latest = 0
                    for i in TABLES[p][1][x, way]:
                        latest = max(latest, i // ROWS)
                        if latest == c:
                            ready.append((way, i))
                if ready:
                    @pl.when(here(p, x))
                    def _():
                        for way, i in ready:
                            pass_on(p, x, way, i, total)

    first_row = lax.broadcasted_iota(jnp.int32, (8, nm), 0) == 0
    last_row = lax.broadcasted_iota(jnp.int32, (8, nm), 0) == 7

    for t in range(STEPS):
        src, dst = bufs[t % 2], bufs[(t + 1) % 2]
        last = t == STEPS - 1

        def chunk(c, _, t=t, src=src, dst=dst, last=last):
            buf = bufs[t % 2]
            arrived("south", xrecv_sem.at[t % 2, c], buf.at[0, pl.ds(1, ROWS)], buf.at[0, pl.ds(1, 2 * ROWS)])
            rows = pl.ds(c * ROWS, ROWS)
            arrived("down", zrecv_sem.at[t % 2, c], zrecv.at[t, 0, rows], zrecv.at[t, pl.ds(0, 2), rows])
            on(jnp.logical_and(has["east"][0], c == 0), lambda: y_copy(t, 1).wait_recv())
            on(jnp.logical_and(has["east"][1], c == chunks - 1), lambda: y_copy(t, 0).wait_recv())

            def row(r, _):
                i = c * ROWS + r
                acc = None
                for j in range(nj):
                    mid = src[1 + j, 1 + i]
                    above = pltpu.roll(mid, 1, 0)
                    under = pltpu.roll(mid, nk - 1, 0)
                    zl = zrecv[t, 0, i, j : j + 1]
                    zh = zrecv[t, 1, i, j : j + 1]
                    above = jnp.concatenate([jnp.where(first_row, zl, above[:8]), above[8:]], axis=0)
                    under = jnp.concatenate([under[:-8], jnp.where(last_row, zh, under[-8:])], axis=0)
                    spread = src[j, 1 + i] + src[2 + j, 1 + i] + src[1 + j, i] + src[1 + j, 2 + i] + above + under - 6.0 * mid
                    new = 2.0 * mid - dst[1 + j, 1 + i] + speed[j, i] * spread
                    dst[1 + j, 1 + i] = new
                    if last:
                        acc = new if acc is None else acc + new
                    else:
                        zsend[t + 1, 0, i, j : j + 1] = new[0:1]
                        zsend[t + 1, 1, i, j : j + 1] = new[nk - 1 : nk]
                if last:
                    total[i] = acc
                return 0

            lax.fori_loop(0, ROWS, row, 0)
            if not last:
                for side in (1, 0):
                    on(has["south"][side], lambda: x_copy(t + 1, side, c).start())
                z_start(t + 1, c)
                on(jnp.logical_and(has["east"][0], c == 0), lambda: y_copy(t + 1, 0).start())
                on(jnp.logical_and(has["east"][1], c == chunks - 1), lambda: y_copy(t + 1, 1).start())
            return 0

        if t >= 1:
            sent_faces(t - 1)
        if last:
            for c in range(chunks):
                chunk(c, 0)
                send_totals(c)
        else:
            lax.fori_loop(0, chunks, chunk, 0)

    for p, x in [(p, x) for p in (0, 1) for x in range(4)]:
        @pl.when(here(p, x))
        def _():
            ways, own, _ = TABLES[p]
            for way, i in relays[p][x]:
                came = landing(x, way, ways[i])
                ring_copy(way, came.at[i], came.at[i], recv[way].at[slots[p][x, way, i]]).wait_recv()
                if x == 3 or (x, way) == (2, "down"):
                    pass_on(p, x, way, i, came)
                else:
                    out = slow if way == "up" else shigh
                    out[i] = came[i] + total[i]
                    pass_on(p, x, way, i, out)
            if x == 2:
                for i in range(ni):
                    if ways[i] == "G":
                        below[i] = ahigh[i] + alow[i]
            for way, w in ENDS[x]:
                rows = [i for i in range(ni) if ways[i] == w]
                ref = total.at[pl.ds(0, len(rows))]
                ring_copy(way, ref, ref, recv[way].at[slots[p][x, way, w]]).wait_recv()
                if landing(x, way, w) is not below:
                    for i in rows:
                        below[i] = ahigh[i] + alow[i]
            if x == 0:
                for i in range(ni):
                    below[i] = jnp.zeros((nk, nm), jnp.float32)
            for way in ("up", "down"):
                count = len(own.get((x, way), ())) + sum(k == way for k, _ in relays[p][x])
                if count:
                    ref = total.at[pl.ds(0, count)]
                    ring_copy(way, ref, ref, uprecv_sem.at[0]).wait_send()

    sent_faces(STEPS - 1)
    for side in (0, 1):
        ref = zsend.at[:, side]
        on(has["down"][side], lambda: remote(ref, ref, zsend_sem.at[side], zrecv_sem.at[0, 0], "down", side).wait_send())


def outputs_kernel(grid_j, field, below, running, end, stage, out_sem, field_sem):
    nj, ni, nk, nm = end.shape
    rows = 2
    groups = ni // rows
    whole = pltpu.make_async_copy(field.at[pl.ds(1, nj), pl.ds(1, ni)], end, field_sem)
    whole.start()

    def out(g):
        at = pl.ds(g * rows, rows)
        return pltpu.make_async_copy(stage.at[:, at], running.at[:, at], out_sem)

    def group(g, _):
        for r in range(rows):
            i = g * rows + r
            acc = below[i]
            for j in range(nj):
                acc = acc + field[1 + j, 1 + i]
                stage[j, i] = acc * (1.0 / grid_j)
        out(g).start()
        return 0

    lax.fori_loop(0, groups, group, 0)

    pltpu.make_async_copy(stage, running, out_sem).wait()
    whole.wait()


def shards(field_now, earlier, speed_square):
    shape = field_now.shape
    nj, ni, nk, nm = shape
    padded = (nj + 2, ni + 2, nk, nm)
    chunks = ni // ROWS
    grid_j = nj * lax.axis_size("south")
    dma = pltpu.SemaphoreType.DMA
    anyspace = pl.BlockSpec(memory_space=pltpu.HBM)
    vmem = pl.BlockSpec(memory_space=pltpu.VMEM)
    f32 = jnp.float32
    field, below = pl.pallas_call(
        functools.partial(steps_kernel, grid_j),
        out_shape=(pltpu.VMEM(padded, f32), pltpu.VMEM((ni, nk, nm), f32)),
        in_specs=[anyspace] * 3,
        out_specs=(vmem, vmem),
        scratch_shapes=[
            pltpu.VMEM(padded, f32),
            pltpu.VMEM(shape, f32),
            pltpu.VMEM((STEPS, 2, ni, nj, nm), f32),
            pltpu.VMEM((STEPS, 2, ni, nj, nm), f32),
            *[pltpu.VMEM((ni, nk, nm), f32)] * 5,
            pltpu.VMEM((2, ROWS, nk, nm), f32),
            dma((4,)),
            dma((2, 2)), dma((2, chunks)),
            dma((2, 2)), dma((2, 2)),
            dma((2,)), dma((2, chunks)),
            dma((2,)), dma((9,)), dma((11,)),
        ],
        compiler_params=pltpu.CompilerParams(
            collective_id=0, has_side_effects=True, vmem_limit_bytes=40 * 1024 * 1024,
        ),
        name="steps",
    )(field_now, earlier, speed_square)
    return pl.pallas_call(
        functools.partial(outputs_kernel, grid_j),
        out_shape=(jax.ShapeDtypeStruct(shape, f32), jax.ShapeDtypeStruct(shape, f32)),
        in_specs=[vmem, vmem],
        out_specs=(anyspace, anyspace),
        scratch_shapes=[pltpu.VMEM(shape, f32), dma, dma],
        compiler_params=pltpu.CompilerParams(vmem_limit_bytes=32 * 1024 * 1024),
        name="outputs",
    )(field, below)


def solution(mesh):
    placed = P(*AXES, None)
    return jax.shard_map(
        shards,
        mesh=mesh,
        in_specs=(placed, placed, placed),
        out_specs=(placed, placed),
        check_vma=False,
    )
```
